1024 devices in a mesh: section: 8 (over z_lo), dp: 32 (over y, x), mp: 4 (over z_hi, core).
Axes of the slice: x: 4, y: 8, z: 16 (z_hi: 2, z_lo: 8; z = z_hi * 8 + z_lo), core: 2. Of those that a mesh axis runs over, the one named last changes fastest.
Arguments:
- fwd_in: bfloat16 [8, 16384, 1024], P('section', ('dp', 'mp')), may hold values from -6 to 6
- stash: bfloat16 [8, 16384, 1024], P('section', ('dp', 'mp')), may hold values from -6 to 6
- cot: bfloat16 [8, 16384, 1024], P('section', ('dp', 'mp')), may hold values from -24 to 24
- w_in: bfloat16 [8, 2048, 1024], P('section', 'mp'), may hold values from -0.1875 to 0.1875
- w_out: bfloat16 [8, 2048, 1024], P('section', 'mp'), may hold values from -0.125 to 0.125
- gain: float32 [8, 1024], P('section'), may hold values from 0.1 to 1.9
Outputs:
- passed_fwd: bfloat16 [8, 16384, 1024], P('section', ('dp', 'mp'))
- passed_grad: bfloat16 [8, 16384, 1024], P('section', ('dp', 'mp'))
- grad_w_in: bfloat16 [8, 2048, 1024], P('section', 'mp', 'dp')
- grad_w_out: bfloat16 [8, 2048, 1024], P('section', 'mp', 'dp')
The draws below stay inside these ranges and needn't reach their ends.
All inputs are finite; a program needn't handle non-finite values.
Results may differ from the reference program's by a relative error of at most 0.015.
Values may be sent and summed in bfloat16 or wider, within the bound.
No kernel may reach another device: no remote copies, remote signals or barrier semaphores. Data moves between devices by JAX's collectives and lax.ppermute only.
A program may use at most 32 MiB of HBM per device.

```python
import jax
import jax.numpy as jnp
from jax import lax

D = 1024
HID = 2048
TOK = 512
HID_DEV = 512
TOKENS = 16384
SECTIONS = 8
N_DP = 32
N_MP = 4


def raised(array, rng, source, target, blocks, factor):
    def block_of(axis_at):
        return (jnp.arange(array.shape[axis_at]) // (array.shape[axis_at] // blocks)).reshape((-1,) + (1,) * (array.ndim - 1 - axis_at))

    one_side = jax.random.permutation(rng, blocks)[block_of(target)]
    other_side = (block_of(target) + blocks // 2) % blocks
    return jnp.where((block_of(source) == one_side) | (block_of(source) == other_side), factor * array, array)


def steps_of(own_key, shape, split, least, high):
    level, own = 1.0, jax.random.fold_in(own_key, 6)
    for position, blocks in split:
        steps = jnp.exp(jax.random.uniform(jax.random.fold_in(own, position), (blocks,), jnp.float32, least / len(split), high / len(split)))
        level = level * jnp.repeat(steps, shape[position] // blocks).reshape([-1 if axis == position else 1 for axis in range(len(shape))])
    return level


def gaussian(key, shape, width, reach, pieces=(), dtype=jnp.bfloat16):
    result = width * jax.random.normal(key, shape, jnp.float32)
    if pieces:
        result = result * steps_of(key, shape, pieces, -0.22, 0.18)
    return jnp.clip(result, -reach, reach).astype(dtype)


def heavy_noise(rng, dims, deviation, most, pieces, heavy, held_as=jnp.bfloat16):
    entries = deviation * jax.random.normal(rng, dims, jnp.float32)
    if pieces:
        entries = entries * steps_of(rng, dims, pieces, -0.22, 0.18)
    return jnp.clip(raised(entries, jax.random.fold_in(rng, 3), *heavy), -most, most).astype(held_as)


def setup_inputs(seed: int = 0) -> dict:
    streams_of = jax.random.split(jax.random.key(seed), 7)
    fwd_in = gaussian(streams_of[0], (SECTIONS, TOKENS, D), 1.0, 6.0, ((0, 8), (1, 128)))
    stash = gaussian(streams_of[1], (SECTIONS, TOKENS, D), 1.0, 6.0, ((0, 8), (1, 128)))
    cot = heavy_noise(streams_of[2], (SECTIONS, TOKENS, D), 1.0, 24.0, ((0, 8), (1, 128)), (1, 2, 128, 5.5))
    w_in = gaussian(streams_of[3], (SECTIONS, HID, D), D ** -0.5, 0.1875, ((0, 8), (1, 4)))
    w_out = gaussian(streams_of[4], (SECTIONS, HID, D), HID ** -0.5, 0.125, ((0, 8), (1, 4)))
    gain = jnp.clip(1.0 + 0.18 * jax.random.normal(streams_of[5], (SECTIONS, D), jnp.float32), 0.1, 1.9)
    return {"fwd_in": fwd_in, "stash": stash, "cot": cot, "w_in": w_in, "w_out": w_out, "gain": gain}


norm_eps = 1e-05
gelu_coef = 0.7978845608

def gelu_value(v):
    inner = jnp.tanh(gelu_coef * (v + 0.044715 * v * v * v))
    return 0.5 * v * (1.0 + inner)

def gelu_slope(v):
    inner = jnp.tanh(gelu_coef * (v + 0.044715 * v * v * v))
    return 0.5 * (1.0 + inner) + 0.5 * v * (1.0 - inner * inner) * gelu_coef * (1.0 + 0.134145 * v * v)

def prepare(x, w_in, gain):
    xf = x.astype(jnp.float32)
    scale = lax.rsqrt(lax.optimization_barrier(jnp.mean(xf * xf, axis=-1, keepdims=True)) + norm_eps)
    normed = (xf * scale * gain[None, :]).astype(jnp.bfloat16)
    pre = lax.dot_general(normed, w_in, (((1,), (1,)), ((), ())), preferred_element_type=jnp.float32)
    act = gelu_value(pre).astype(jnp.bfloat16)
    return (xf, scale, normed, pre, act)

def group_sum(left, right):
    rows = left.shape[0]
    lhs = left.reshape(rows, N_MP, HID_DEV).astype(jnp.float32)
    rhs = right.reshape(N_MP, HID_DEV, right.shape[1]).astype(jnp.float32)
    parts = jnp.einsum('tgh,ghd->gtd', lhs, rhs).astype(jnp.bfloat16)
    parts = lax.optimization_barrier(parts)
    return lax.optimization_barrier(jnp.sum(parts.astype(jnp.float32), axis=0))

def replica_sum(left, right):
    lhs = left.reshape(N_DP, TOK, left.shape[1]).astype(jnp.float32)
    rhs = right.reshape(N_DP, TOK, right.shape[1]).astype(jnp.float32)
    parts = jnp.einsum('rth,rtd->rhd', lhs, rhs).astype(jnp.bfloat16)
    parts = lax.optimization_barrier(parts)
    return lax.optimization_barrier(jnp.sum(parts.astype(jnp.float32), axis=0)).astype(jnp.bfloat16)

def reference(fwd_in, stash, cot, w_in, w_out, gain):
    outs = []
    grads = []
    g_ins = []
    g_outs = []
    for section in range(SECTIONS):
        xf, scale, normed, pre, act = prepare(fwd_in[section], w_in[section], gain[section])
        outs.append((xf + group_sum(act, w_out[section])).astype(jnp.bfloat16))
        sf, sscale, snormed, spre, sact = prepare(stash[section], w_in[section], gain[section])
        cot_rows = cot[section]
        d_act = lax.dot_general(cot_rows, w_out[section], (((1,), (1,)), ((), ())), preferred_element_type=jnp.float32)
        d_pre = (d_act * gelu_slope(spre)).astype(jnp.bfloat16)
        d_norm = group_sum(d_pre, w_in[section])
        push = d_norm * gain[section][None, :]
        mixed = lax.optimization_barrier(jnp.mean(sf * push, axis=-1, keepdims=True))
        dx = cot_rows.astype(jnp.float32) + sscale * push - sf * sscale * sscale * sscale * mixed
        grads.append(dx.astype(jnp.bfloat16))
        g_outs.append(replica_sum(sact, cot_rows))
        g_ins.append(replica_sum(d_pre, snormed))
    passed_fwd = jnp.roll(jnp.stack(outs), 1, axis=0)
    passed_grad = jnp.roll(jnp.stack(grads), -1, axis=0)
    return (passed_fwd, passed_grad, jnp.stack(g_ins), jnp.stack(g_outs))
```

```python
import jax
import jax.numpy as jnp
from jax import lax
from jax.sharding import PartitionSpec as P


norm_eps = 1e-05
gelu_coef = 0.7978845608


NX, NY = 4, 8
x_groups = [[NX * y + x for x in range(NX)] for y in range(NY)]
y_groups = [[NX * y + x for y in range(NY)] for x in range(NX)]
other_chip = [(0, 2), (1, 3), (2, 0), (3, 1)]
other_core = [(0, 1), (1, 0), (2, 3), (3, 2)]

f32, bf16 = jnp.float32, jnp.bfloat16


def to_chip(x):
    return lax.ppermute(x, "mp", other_chip)


def to_core(x):
    return lax.ppermute(x, "mp", other_core)


def shifted(x, axis, by):
    length = lax.axis_size(axis)
    return lax.ppermute(x, axis, [(i, (i + by) % length) for i in range(length)])


def gathered(x, groups):
    copies = jnp.broadcast_to(x, (len(groups[0]), *x.shape))
    return lax.all_to_all(copies, "dp", 0, 0, tiled=True, axis_index_groups=groups)


def summed(x, groups):
    pieces = lax.all_to_all(x, "dp", 0, 0, tiled=True, axis_index_groups=groups)
    return jnp.sum(pieces.astype(f32), axis=0)


def gelu_both(v):
    t = jnp.tanh(gelu_coef * (v + 0.044715 * v * v * v))
    value = 0.5 * v * (1.0 + t)
    slope = 0.5 * (1.0 + t) + 0.5 * v * (1.0 - t * t) * gelu_coef * (1.0 + 0.134145 * v * v)
    return value, slope


def scale_of(x):
    xf = x.astype(f32)
    return lax.rsqrt(jnp.mean(xf * xf, axis=-1, keepdims=True) + norm_eps)


def norm(x, gain_row):
    return (x.astype(f32) * scale_of(x) * gain_row[None, :]).astype(bf16)


def nt(a, b):
    return lax.dot_general(a, b, (((1,), (1,)), ((), ())), preferred_element_type=f32)


def tn(a, b):
    return lax.dot_general(a, b, (((0,), (0,)), ((), ())), preferred_element_type=f32)


def nn(a, b):
    return jnp.dot(a, b, preferred_element_type=f32)


def layer(fwd_in, stash, cot, w_in, w_out, gain):
    xf, xb, ct = fwd_in[0], stash[0], cot[0]
    wi, wo, gain_row = w_in[0], w_out[0], gain[0]
    rows = xf.shape[0]
    n_dp = lax.axis_size("dp")
    d = lax.axis_index("dp")
    part = wi.shape[0] // n_dp
    at = (d % NX * NY + d // NX) * part
    mine = jnp.stack(
        [lax.dynamic_slice_in_dim(wi, at, part, 0), lax.dynamic_slice_in_dim(wo, at, part, 0)]
    )
    piece = to_chip(mine)
    far = to_chip(jnp.concatenate([xb, ct]))
    near = to_core(jnp.concatenate([xf, xb, ct]))
    f2 = jnp.concatenate([xf, near[:rows]])
    b2 = jnp.concatenate([xb, near[rows : 2 * rows]])
    c2 = jnp.concatenate([ct, near[2 * rows :]])
    nf, nb = norm(f2, gain_row), norm(b2, gain_row)
    act_f, _ = gelu_both(nt(nf, wi))
    branch = nn(act_f.astype(bf16), wo)
    act_b, slope_b = gelu_both(nt(nb, wi))
    d_pre = (nt(c2, wo) * slope_b).astype(bf16)
    d_norm = nn(d_pre, wi)
    col = gathered(piece, y_groups)
    whole = gathered(col.reshape(NY, 2, part, -1), x_groups).reshape(n_dp, 2, part, -1)
    wi2 = whole[:, 0].reshape(wi.shape)
    wo2 = whole[:, 1].reshape(wo.shape)
    act_f2, _ = gelu_both(nt(nf, wi2))
    branch = branch + nn(act_f2.astype(bf16), wo2)
    branch = branch[:rows] + to_core(branch[rows:].astype(bf16)).astype(f32)
    out = (xf.astype(f32) + branch).astype(bf16)
    passed_fwd = shifted(out, "section", 1)
    _, slope_b2 = gelu_both(nt(nb, wi2))
    d_pre2 = (nt(c2, wo2) * slope_b2).astype(bf16)
    d_norm = d_norm + nn(d_pre2, wi2)
    d_norm = d_norm[:rows] + to_core(d_norm[rows:].astype(bf16)).astype(f32)
    scale = scale_of(xb)
    shard_x = xb.astype(f32)
    push = d_norm * gain_row[None, :]
    mixed = jnp.mean(shard_x * push, axis=-1, keepdims=True)
    dx = ct.astype(f32) + scale * push - shard_x * scale * scale * scale * mixed
    passed_grad = shifted(dx.astype(bf16), "section", -1)
    far2 = to_core(far)
    b3 = jnp.concatenate([far[:rows], far2[:rows]])
    c3 = jnp.concatenate([far[rows:], far2[rows:]])
    nb3 = norm(b3, gain_row)
    act_b3, slope_b3 = gelu_both(nt(nb3, wi))
    d_pre3 = (nt(c3, wo) * slope_b3).astype(bf16)
    g_in = tn(jnp.concatenate([nb, nb3]), jnp.concatenate([d_pre, d_pre3]))
    g_out = tn(
        jnp.concatenate([c2, c3]), jnp.concatenate([act_b.astype(bf16), act_b3.astype(bf16)])
    )
    hid = wi.shape[0]
    g = jnp.concatenate([g_in.astype(bf16), g_out.astype(bf16)], axis=1)
    g = g.reshape(NY, NX, -1, 2 * hid).swapaxes(0, 1)
    g = summed(g, x_groups).astype(bf16)
    g = summed(g, y_groups).astype(bf16)
    return (passed_fwd[None], passed_grad[None], g[:, :hid].T[None], g[:, hid:].T[None])


def solution(mesh):
    in_specs = (
        P("section", ("dp", "mp"), None),
        P("section", ("dp", "mp"), None),
        P("section", ("dp", "mp"), None),
        P("section", "mp", None),
        P("section", "mp", None),
        P("section", None),
    )
    out_specs = (
        P("section", ("dp", "mp"), None),
        P("section", ("dp", "mp"), None),
        P("section", "mp", "dp"),
        P("section", "mp", "dp"),
    )
    return jax.shard_map(layer, mesh=mesh, in_specs=in_specs, out_specs=out_specs, check_vma=False)
```

```python
import jax
import jax.numpy as jnp
from jax import lax
from jax.experimental import pallas as pl
from jax.experimental.pallas import tpu as pltpu
from jax.sharding import PartitionSpec as P


norm_eps = 1e-05
gelu_coef = 0.7978845608


NX, NY = 4, 8
x_groups = [[NX * y + x for x in range(NX)] for y in range(NY)]
y_groups = [[NX * y + x for y in range(NY)] for x in range(NX)]
other_chip = [(0, 2), (1, 3), (2, 0), (3, 1)]
other_core = [(0, 1), (1, 0), (2, 3), (3, 2)]

f32, bf16 = jnp.float32, jnp.bfloat16
CHUNK = 32
TILE = 256


def to_chip(x):
    return lax.ppermute(x, "mp", other_chip)


def to_core(x):
    return lax.ppermute(x, "mp", other_core)


def shifted(x, axis, by):
    length = lax.axis_size(axis)
    return lax.ppermute(x, axis, [(i, (i + by) % length) for i in range(length)])


def gathered(x, groups):
    copies = jnp.broadcast_to(x, (len(groups[0]), *x.shape))
    return lax.all_to_all(copies, "dp", 0, 0, tiled=True, axis_index_groups=groups)


def exchanged(x, groups):
    return lax.all_to_all(x, "dp", 0, 0, tiled=True, axis_index_groups=groups)


def gelu_both(v):
    t = jnp.tanh(gelu_coef * (v + 0.044715 * v * v * v))
    value = 0.5 * v * (1.0 + t)
    slope = 0.5 * (1.0 + t) + 0.5 * v * (1.0 - t * t) * gelu_coef * (1.0 + 0.134145 * v * v)
    return value, slope


def scale_of(xf):
    return lax.rsqrt(jnp.mean(xf * xf, axis=-1, keepdims=True) + norm_eps)


def nt(a, b):
    return lax.dot_general(a, b, (((1,), (1,)), ((), ())), preferred_element_type=f32)


def tn(a, b):
    return lax.dot_general(a, b, (((0,), (0,)), ((), ())), preferred_element_type=f32)


def nn(a, b):
    return jnp.dot(a, b, preferred_element_type=f32)


def norm_into(src, at, gain, dst, to, rows):
    def step(i, _):
        r = pl.multiple_of(i * CHUNK, CHUNK)
        x = src[pl.ds(at + r, CHUNK), :].astype(f32)
        dst[pl.ds(to + r, CHUNK), :] = (x * scale_of(x) * gain[...]).astype(bf16)

    lax.fori_loop(0, rows // CHUNK, step, None)


def own_kernel(xf, xb, ct, near, wi, wo, gain, nf, nb, c2, act, dp, br, dn, act_f):
    rows = xf.shape[0]
    norm_into(xf, 0, gain, nf, 0, rows)
    norm_into(near, 0, gain, nf, rows, rows)
    norm_into(xb, 0, gain, nb, 0, rows)
    norm_into(near, rows, gain, nb, rows, rows)
    c2[:rows, :] = ct[...]
    c2[rows:, :] = near[2 * rows :, :]

    def hidden(j, _):
        h = pl.ds(pl.multiple_of(j * TILE, TILE), TILE)
        value, _ = gelu_both(nt(nf[...], wi[h, :]))
        act_f[:, h] = value.astype(bf16)
        value, slope = gelu_both(nt(nb[...], wi[h, :]))
        act[:, h] = value.astype(bf16)
        dp[:, h] = (nt(c2[...], wo[h, :]) * slope).astype(bf16)

    lax.fori_loop(0, wi.shape[0] // TILE, hidden, None)

    def back(j, _):
        c = pl.ds(pl.multiple_of(j * TILE, TILE), TILE)
        br[:, c] = nn(act_f[...], wo[:, c])
        dn[:, c] = nn(dp[...], wi[:, c])

    lax.fori_loop(0, wi.shape[1] // TILE, back, None)


def rest_kernel(whole, nf, nb, c2, br, dn, keep, send, act_f, dp, wi, wo):
    rows = keep.shape[1]

    def split(i, _):
        r = pl.ds(pl.multiple_of(i * 16, 16), 16)
        wi[r, :] = whole[i, 0]
        wo[r, :] = whole[i, 1]

    lax.fori_loop(0, whole.shape[0], split, None)

    def hidden(j, _):
        h = pl.ds(pl.multiple_of(j * TILE, TILE), TILE)
        value, _ = gelu_both(nt(nf[...], wi[h, :]))
        act_f[:, h] = value.astype(bf16)
        _, slope = gelu_both(nt(nb[...], wi[h, :]))
        dp[:, h] = (nt(c2[...], wo[h, :]) * slope).astype(bf16)

    lax.fori_loop(0, wi.shape[0] // TILE, hidden, None)

    def back(j, _):
        c = pl.ds(pl.multiple_of(j * TILE, TILE), TILE)
        b = br[:, c] + nn(act_f[...], wo[:, c])
        keep[0, :, c] = b[:rows]
        send[0, :, c] = b[rows:].astype(bf16)
        g = dn[:, c] + nn(dp[...], wi[:, c])
        keep[1, :, c] = g[:rows]
        send[1, :, c] = g[rows:].astype(bf16)

    lax.fori_loop(0, wi.shape[1] // TILE, back, None)


def grad_kernel(far, far2, wi, wo, gain, nb, c2, act, dp, g, nb3, c3, act3, dp3):
    rows = far.shape[0] // 2
    hid = wi.shape[0]
    norm_into(far, 0, gain, nb3, 0, rows)
    norm_into(far2, 0, gain, nb3, rows, rows)
    c3[:rows, :] = far[rows:, :]
    c3[rows:, :] = far2[rows:, :]

    def hidden(j, _):
        h = pl.ds(pl.multiple_of(j * TILE, TILE), TILE)
        value, slope = gelu_both(nt(nb3[...], wi[h, :]))
        act3[:, h] = value.astype(bf16)
        dp3[:, h] = (nt(c3[...], wo[h, :]) * slope).astype(bf16)

    lax.fori_loop(0, hid // TILE, hidden, None)

    def grads(y, _):
        c = pl.ds(pl.multiple_of(y * 128, 128), 128)
        gi = tn(nb[:, c], dp[...]) + tn(nb3[:, c], dp3[...])
        g[:, y, :, :hid] = gi.astype(bf16).reshape(NX, 32, hid)
        go = tn(c2[:, c], act[...]) + tn(c3[:, c], act3[...])
        g[:, y, :, hid:] = go.astype(bf16).reshape(NX, 32, hid)

    lax.fori_loop(0, NY, grads, None)


def sum_kernel(pieces, total):
    total[...] = jnp.sum(pieces[...].astype(f32), axis=0).astype(bf16)


def local(kernel, outs, scratch, flops, moved):
    return pl.pallas_call(
        kernel,
        out_shape=[jax.ShapeDtypeStruct(s, t) for s, t in outs],
        scratch_shapes=[pltpu.VMEM(s, t) for s, t in scratch],
        compiler_params=pltpu.CompilerParams(vmem_limit_bytes=28 * 2**20),
        cost_estimate=pl.CostEstimate(flops=flops, bytes_accessed=moved, transcendentals=0),
    )


def layer(fwd_in, stash, cot, w_in, w_out, gain):
    xf, xb, ct = fwd_in[0], stash[0], cot[0]
    wi, wo = w_in[0], w_out[0]
    rows, dim = xf.shape
    hid = wi.shape[0]
    both = 2 * rows
    n_dp = lax.axis_size("dp")
    d = lax.axis_index("dp")
    part = hid // n_dp
    at = (d % NX * NY + d // NX) * part
    mine = jnp.stack(
        [lax.dynamic_slice_in_dim(wi, at, part, 0), lax.dynamic_slice_in_dim(wo, at, part, 0)]
    )
    piece = to_chip(mine)
    far = to_chip(jnp.concatenate([xb, ct]))
    near = to_core(jnp.concatenate([xf, xb, ct]))
    nf, nb, c2, act, dp, br, dn = local(
        own_kernel,
        [((both, dim), bf16)] * 3 + [((both, hid), bf16)] * 2 + [((both, dim), f32)] * 2,
        [((both, hid), bf16)],
        10 * both * hid * dim,
        8 * 2**20,
    )(xf, xb, ct, near, wi, wo, gain)
    col = gathered(piece, y_groups)
    whole = gathered(col, x_groups).reshape(n_dp, 2, part, dim)
    keep, send = local(
        rest_kernel,
        [((2, rows, dim), f32), ((2, rows, dim), bf16)],
        [((both, hid), bf16)] * 2 + [((hid, dim), bf16)] * 2,
        10 * both * hid * dim,
        8 * 2**20,
    )(whole, nf, nb, c2, br, dn)
    sums = keep + to_core(send).astype(f32)
    out = (xf.astype(f32) + sums[0]).astype(bf16)
    passed_fwd = shifted(out, "section", 1)
    shard_x = xb.astype(f32)
    scale = scale_of(shard_x)
    push = sums[1] * gain
    mixed = jnp.mean(shard_x * push, axis=-1, keepdims=True)
    dx = ct.astype(f32) + scale * push - shard_x * scale * scale * scale * mixed
    passed_grad = shifted(dx.astype(bf16), "section", -1)
    far2 = to_core(far)
    (g,) = local(
        grad_kernel,
        [((NX, NY, dim // n_dp, 2 * hid), bf16)],
        [((both, dim), bf16)] * 2 + [((both, hid), bf16)] * 2,
        12 * both * hid * dim,
        8 * 2**20,
    )(far, far2, wi, wo, gain, nb, c2, act, dp)
    g = exchanged(g, x_groups)
    g = pl.pallas_call(
        sum_kernel,
        grid=(NY,),
        in_specs=[pl.BlockSpec((NX, 1, *g.shape[2:]), lambda i: (0, i, 0, 0))],
        out_specs=pl.BlockSpec((1, *g.shape[2:]), lambda i: (i, 0, 0)),
        out_shape=jax.ShapeDtypeStruct(g.shape[1:], bf16),
        compiler_params=pltpu.CompilerParams(vmem_limit_bytes=16 * 2**20),
        cost_estimate=pl.CostEstimate(flops=2**21, bytes_accessed=2**21, transcendentals=0),
    )(g)
    g = exchanged(g, y_groups)
    g = jnp.sum(g.astype(f32), axis=0).astype(bf16)
    return (passed_fwd[None], passed_grad[None], g[:, :hid].T[None], g[:, hid:].T[None])


def solution(mesh):
    in_specs = (
        P("section", ("dp", "mp"), None),
        P("section", ("dp", "mp"), None),
        P("section", ("dp", "mp"), None),
        P("section", "mp", None),
        P("section", "mp", None),
        P("section", None),
    )
    out_specs = (
        P("section", ("dp", "mp"), None),
        P("section", ("dp", "mp"), None),
        P("section", "mp", "dp"),
        P("section", "mp", "dp"),
    )
    return jax.shard_map(layer, mesh=mesh, in_specs=in_specs, out_specs=out_specs, check_vma=False)
```

```python
import jax
import jax.numpy as jnp
from jax import lax
from jax.experimental import pallas as pl
from jax.experimental.pallas import tpu as pltpu
from jax.sharding import PartitionSpec as P


norm_eps = 1e-05
gelu_coef = 0.7978845608


NEAR, FAR = 8, 4
near_groups = [[NEAR * k + j for j in range(NEAR)] for k in range(FAR)]
far_groups = [[NEAR * k + j for k in range(FAR)] for j in range(NEAR)]
other_chip = [(0, 2), (1, 3), (2, 0), (3, 1)]
other_core = [(0, 1), (1, 0), (2, 3), (3, 2)]

f32, bf16 = jnp.float32, jnp.bfloat16
CHUNK = 32
TILE = 256


def to_chip(x):
    return lax.ppermute(x, "mp", other_chip)


def to_core(x):
    return lax.ppermute(x, "mp", other_core)


def shifted(x, axis, by):
    length = lax.axis_size(axis)
    return lax.ppermute(x, axis, [(i, (i + by) % length) for i in range(length)])


def gathered(x, groups):
    copies = jnp.broadcast_to(x, (len(groups[0]), *x.shape))
    return lax.all_to_all(copies, "dp", 0, 0, tiled=True, axis_index_groups=groups)


def exchanged(x, groups):
    return lax.all_to_all(x, "dp", 0, 0, tiled=True, axis_index_groups=groups)


def gelu_both(v):
    t = jnp.tanh(gelu_coef * (v + 0.044715 * v * v * v))
    value = 0.5 * v * (1.0 + t)
    slope = 0.5 * (1.0 + t) + 0.5 * v * (1.0 - t * t) * gelu_coef * (1.0 + 0.134145 * v * v)
    return value, slope


def scale_of(xf):
    return lax.rsqrt(jnp.mean(xf * xf, axis=-1, keepdims=True) + norm_eps)


def nt(a, b):
    return lax.dot_general(a, b, (((1,), (1,)), ((), ())), preferred_element_type=f32)


def tn(a, b):
    return lax.dot_general(a, b, (((0,), (0,)), ((), ())), preferred_element_type=f32)


def nn(a, b):
    return jnp.dot(a, b, preferred_element_type=f32)


def norm_into(src, at, gain, dst, to, rows):
    def step(i, _):
        r = pl.multiple_of(i * CHUNK, CHUNK)
        x = src[pl.ds(at + r, CHUNK), :].astype(f32)
        dst[pl.ds(to + r, CHUNK), :] = (x * scale_of(x) * gain[...]).astype(bf16)

    lax.fori_loop(0, rows // CHUNK, step, None)


def own_kernel(xf, xb, ct, near, wi, wo, gain, nf, nb, c2, br, dn, p, act_f, act, dp):
    rows = xf.shape[0]
    hid = wi.shape[0]
    norm_into(xf, 0, gain, nf, 0, rows)
    norm_into(near, 0, gain, nf, rows, rows)
    norm_into(xb, 0, gain, nb, 0, rows)
    norm_into(near, rows, gain, nb, rows, rows)
    c2[:rows, :] = ct[...]
    c2[rows:, :] = near[2 * rows :, :]

    def hidden(j, _):
        h = pl.ds(pl.multiple_of(j * TILE, TILE), TILE)
        value, _ = gelu_both(nt(nf[...], wi[h, :]))
        act_f[:, h] = value.astype(bf16)
        value, slope = gelu_both(nt(nb[...], wi[h, :]))
        act[:, h] = value.astype(bf16)
        dp[:, h] = (nt(c2[...], wo[h, :]) * slope).astype(bf16)

    lax.fori_loop(0, wi.shape[0] // TILE, hidden, None)

    def back(j, _):
        c = pl.ds(pl.multiple_of(j * TILE, TILE), TILE)
        br[:, c] = nn(act_f[...], wo[:, c])
        dn[:, c] = nn(dp[...], wi[:, c])
        p[c, :hid] = tn(nb[:, c], dp[...])
        p[c, hid:] = tn(c2[:, c], act[...])

    lax.fori_loop(0, wi.shape[1] // TILE, back, None)


def rest_kernel(whole, nf, nb, c2, br, dn, keep, send, act_f, dp, wi, wo):
    rows = keep.shape[1]

    def split(i, _):
        r = pl.ds(pl.multiple_of(i * 16, 16), 16)
        wi[r, :] = whole[i, 0]
        wo[r, :] = whole[i, 1]

    lax.fori_loop(0, whole.shape[0], split, None)

    def hidden(j, _):
        h = pl.ds(pl.multiple_of(j * TILE, TILE), TILE)
        value, _ = gelu_both(nt(nf[...], wi[h, :]))
        act_f[:, h] = value.astype(bf16)
        _, slope = gelu_both(nt(nb[...], wi[h, :]))
        dp[:, h] = (nt(c2[...], wo[h, :]) * slope).astype(bf16)

    lax.fori_loop(0, wi.shape[0] // TILE, hidden, None)

    def back(j, _):
        c = pl.ds(pl.multiple_of(j * TILE, TILE), TILE)
        b = br[:, c] + nn(act_f[...], wo[:, c])
        keep[0, :, c] = b[:rows]
        send[0, :, c] = b[rows:].astype(bf16)
        g = dn[:, c] + nn(dp[...], wi[:, c])
        keep[1, :, c] = g[:rows]
        send[1, :, c] = g[rows:].astype(bf16)

    lax.fori_loop(0, wi.shape[1] // TILE, back, None)


def grad_kernel(far, far2, wi, wo, gain, p, g, vfar, vwi, vwo, vp, vg, nb3, c3, act3, dp3, arrived, sent):
    rows = far.shape[0] // 2
    hid = wi.shape[0]
    loads = [
        pltpu.make_async_copy(src, dst, arrived.at[i])
        for i, (src, dst) in enumerate(
            [(far, vfar.at[0]), (far2, vfar.at[1]), (wi, vwi), (wo, vwo), (p, vp)]
        )
    ]
    for load in loads:
        load.start()
    for k in range(2):
        loads[k].wait()
        norm_into(vfar.at[k], 0, gain, nb3, k * rows, rows)
        c3[k * rows : (k + 1) * rows, :] = vfar[k, rows:, :]
    loads[2].wait()
    loads[3].wait()

    def hidden(j, _):
        h = pl.ds(pl.multiple_of(j * TILE, TILE), TILE)
        value, slope = gelu_both(nt(nb3[...], vwi[h, :]))
        act3[:, h] = value.astype(bf16)
        dp3[:, h] = (nt(c3[...], vwo[h, :]) * slope).astype(bf16)

    lax.fori_loop(0, hid // TILE, hidden, None)
    loads[4].wait()
    stores = []
    for k in range(FAR):
        c = slice(k * TILE, (k + 1) * TILE)
        gi = vp[c, :hid] + tn(nb3[:, c], dp3[...])
        vg[:, k, :, :hid] = gi.astype(bf16).reshape(NEAR, -1, hid)
        go = vp[c, hid:] + tn(c3[:, c], act3[...])
        vg[:, k, :, hid:] = go.astype(bf16).reshape(NEAR, -1, hid)
        store = pltpu.make_async_copy(vg.at[:, k], g.at[:, k], sent.at[k])
        store.start()
        stores.append(store)
    for store in stores:
        store.wait()


def sum_kernel(pieces, total):
    def step(k, _):
        total[k] = jnp.sum(pieces[:, k].astype(f32), axis=0).astype(bf16)

    lax.fori_loop(0, pieces.shape[1], step, None)


def last_kernel(pieces, g_in, g_out):
    hid = g_in.shape[1]
    total = jnp.sum(pieces[...].astype(f32), axis=0).astype(bf16)
    g_in[...] = total[:, :hid]
    g_out[...] = total[:, hid:]


def landed_kernel(a, b, c, d):
    c[0] = a[...]
    d[0] = b[...]


def local(kernel, outs, scratch, flops, moved, mib=56, **specs):
    return pl.pallas_call(
        kernel,
        out_shape=[jax.ShapeDtypeStruct(s, t) for s, t in outs],
        scratch_shapes=[pltpu.VMEM(*a) if isinstance(a, tuple) else a for a in scratch],
        compiler_params=pltpu.CompilerParams(vmem_limit_bytes=mib * 2**20),
        cost_estimate=pl.CostEstimate(flops=flops, bytes_accessed=moved, transcendentals=0),
        **specs,
    )


def layer(fwd_in, stash, cot, w_in, w_out, gain):
    xf, xb, ct = fwd_in[0], stash[0], cot[0]
    wi, wo = w_in[0], w_out[0]
    rows, dim = xf.shape
    hid = wi.shape[0]
    both = 2 * rows
    n_dp = lax.axis_size("dp")
    d = lax.axis_index("dp")
    part = hid // n_dp
    at = (d % NEAR * FAR + d // NEAR) * part
    mine = jnp.stack(
        [lax.dynamic_slice_in_dim(wi, at, part, 0), lax.dynamic_slice_in_dim(wo, at, part, 0)]
    )
    piece = to_chip(mine)
    far = to_chip(jnp.concatenate([xb, ct]))
    near = to_core(jnp.concatenate([xf, xb, ct]))
    nf, nb, c2, br, dn, p = local(
        own_kernel,
        [((both, dim), bf16)] * 3 + [((both, dim), f32)] * 2 + [((dim, 2 * hid), f32)],
        [((both, hid), bf16)] * 3,
        14 * both * hid * dim,
        11 * 2**20,
    )(xf, xb, ct, near, wi, wo, gain)
    col = gathered(piece, far_groups)
    whole = gathered(col, near_groups).reshape(n_dp, 2, part, dim)
    keep, send = local(
        rest_kernel,
        [((2, rows, dim), f32), ((2, rows, dim), bf16)],
        [((both, hid), bf16)] * 2 + [((hid, dim), bf16)] * 2,
        10 * both * hid * dim,
        8 * 2**20,
    )(whole, nf, nb, c2, br, dn)
    sums = keep + to_core(send).astype(f32)
    out = (xf.astype(f32) + sums[0]).astype(bf16)
    passed_fwd = shifted(out, "section", 1)
    shard_x = xb.astype(f32)
    scale = scale_of(shard_x)
    push = sums[1] * gain
    mixed = jnp.mean(shard_x * push, axis=-1, keepdims=True)
    dx = ct.astype(f32) + scale * push - shard_x * scale * scale * scale * mixed
    passed_grad = shifted(dx.astype(bf16), "section", -1)
    far2 = to_core(far)
    cut = dim // n_dp
    (g,) = local(
        grad_kernel,
        [((NEAR, FAR, cut, 2 * hid), bf16)],
        [
            ((2, both, dim), bf16),
            ((hid, dim), bf16),
            ((hid, dim), bf16),
            ((dim, 2 * hid), f32),
            ((NEAR, FAR, cut, 2 * hid), bf16),
            ((both, dim), bf16),
            ((both, dim), bf16),
            ((both, hid), bf16),
            ((both, hid), bf16),
            pltpu.SemaphoreType.DMA((5,)),
            pltpu.SemaphoreType.DMA((FAR,)),
        ],
        8 * both * hid * dim,
        9 * 2**20,
        in_specs=[pl.BlockSpec(memory_space=pl.ANY)] * 4
        + [pl.BlockSpec(memory_space=pltpu.VMEM), pl.BlockSpec(memory_space=pl.ANY)],
        out_specs=[pl.BlockSpec(memory_space=pl.ANY)],
    )(far, far2, wi, wo, gain, p)
    g = exchanged(g, near_groups)
    (g,) = local(sum_kernel, [(g.shape[1:], bf16)], [], 2**21, 2**21, mib=16)(g)
    g = exchanged(g, far_groups)
    passed_fwd, passed_grad = local(
        landed_kernel, [((1, rows, dim), bf16)] * 2, [], 2**20, 2**20, mib=16
    )(passed_fwd, passed_grad)
    g_in, g_out = local(last_kernel, [((cut, hid), bf16)] * 2, [], 2**18, 2**18, mib=16)(g)
    return passed_fwd, passed_grad, g_in.T[None], g_out.T[None]


def solution(mesh):
    in_specs = (
        P("section", ("dp", "mp"), None),
        P("section", ("dp", "mp"), None),
        P("section", ("dp", "mp"), None),
        P("section", "mp", None),
        P("section", "mp", None),
        P("section", None),
    )
    out_specs = (
        P("section", ("dp", "mp"), None),
        P("section", ("dp", "mp"), None),
        P("section", "mp", "dp"),
        P("section", "mp", "dp"),
    )
    return jax.shard_map(layer, mesh=mesh, in_specs=in_specs, out_specs=out_specs, check_vma=False)
```

```python
import jax
import jax.numpy as jnp
from jax import lax
from jax.experimental import pallas as pl
from jax.experimental.pallas import tpu as pltpu
from jax.sharding import PartitionSpec as P


norm_eps = 1e-05
gelu_coef = 0.7978845608


NEAR, FAR = 8, 4
near_groups = [[NEAR * k + j for j in range(NEAR)] for k in range(FAR)]
far_groups = [[NEAR * k + j for k in range(FAR)] for j in range(NEAR)]
other_chip = [(0, 2), (1, 3), (2, 0), (3, 1)]
other_core = [(0, 1), (1, 0), (2, 3), (3, 2)]

f32, bf16 = jnp.float32, jnp.bfloat16
vmem = pl.BlockSpec(memory_space=pltpu.VMEM)
hbm = pl.BlockSpec(memory_space=pltpu.HBM)
CHUNK = 32
TILE = 256


def to_chip(x):
    return lax.ppermute(x, "mp", other_chip)


def to_core(x):
    return lax.ppermute(x, "mp", other_core)


def shifted(x, axis, by):
    length = lax.axis_size(axis)
    return lax.ppermute(x, axis, [(i, (i + by) % length) for i in range(length)])


def gathered(x, groups):
    copies = jnp.broadcast_to(x, (len(groups[0]), *x.shape))
    return lax.all_to_all(copies, "dp", 0, 0, tiled=True, axis_index_groups=groups)


def exchanged(x, groups):
    return lax.all_to_all(x, "dp", 0, 0, tiled=True, axis_index_groups=groups)


def gelu_both(v):
    t = jnp.tanh(gelu_coef * (v + 0.044715 * v * v * v))
    value = 0.5 * v * (1.0 + t)
    slope = 0.5 * (1.0 + t) + 0.5 * v * (1.0 - t * t) * gelu_coef * (1.0 + 0.134145 * v * v)
    return value, slope


def scale_of(xf):
    return lax.rsqrt(jnp.mean(xf * xf, axis=-1, keepdims=True) + norm_eps)


def nt(a, b):
    return lax.dot_general(a, b, (((1,), (1,)), ((), ())), preferred_element_type=f32)


def tn(a, b):
    return lax.dot_general(a, b, (((0,), (0,)), ((), ())), preferred_element_type=f32)


def nn(a, b):
    return jnp.dot(a, b, preferred_element_type=f32)


def norm_into(src, at, gain, dst, to, rows):
    def step(i, _):
        r = pl.multiple_of(i * CHUNK, CHUNK)
        x = src[pl.ds(at + r, CHUNK), :].astype(f32)
        dst[pl.ds(to + r, CHUNK), :] = (x * scale_of(x) * gain[...]).astype(bf16)

    lax.fori_loop(0, rows // CHUNK, step, None)


def own_kernel(xf, xb, ct, near, wi, wo, gain, nf, nb, c2, br, dn, p, act_f, act, dp):
    rows = xf.shape[0]
    hid = wi.shape[0]
    norm_into(xf, 0, gain, nf, 0, rows)
    norm_into(near, 0, gain, nf, rows, rows)
    norm_into(xb, 0, gain, nb, 0, rows)
    norm_into(near, rows, gain, nb, rows, rows)
    c2[:rows, :] = ct[...]
    c2[rows:, :] = near[2 * rows :, :]

    def hidden(j, _):
        h = pl.ds(pl.multiple_of(j * TILE, TILE), TILE)
        value, _ = gelu_both(nt(nf[...], wi[h, :]))
        act_f[:, h] = value.astype(bf16)
        value, slope = gelu_both(nt(nb[...], wi[h, :]))
        act[:, h] = value.astype(bf16)
        dp[:, h] = (nt(c2[...], wo[h, :]) * slope).astype(bf16)

    lax.fori_loop(0, wi.shape[0] // TILE, hidden, None)

    def back(j, _):
        c = pl.ds(pl.multiple_of(j * TILE, TILE), TILE)
        br[:, c] = nn(act_f[...], wo[:, c])
        dn[:, c] = nn(dp[...], wi[:, c])
        p[c, :hid] = tn(nb[:, c], dp[...])
        p[c, hid:] = tn(c2[:, c], act[...])

    lax.fori_loop(0, wi.shape[1] // TILE, back, None)


def rest_kernel(whole, nf, nb, c2, br, dn, keep, send, act_f, dp, wi, wo):
    rows = keep.shape[1]

    def split(i, _):
        r = pl.ds(pl.multiple_of(i * 16, 16), 16)
        wi[r, :] = whole[i, 0]
        wo[r, :] = whole[i, 1]

    lax.fori_loop(0, whole.shape[0], split, None)

    def hidden(j, _):
        h = pl.ds(pl.multiple_of(j * TILE, TILE), TILE)
        value, _ = gelu_both(nt(nf[...], wi[h, :]))
        act_f[:, h] = value.astype(bf16)
        _, slope = gelu_both(nt(nb[...], wi[h, :]))
        dp[:, h] = (nt(c2[...], wo[h, :]) * slope).astype(bf16)

    lax.fori_loop(0, wi.shape[0] // TILE, hidden, None)

    def back(j, _):
        c = pl.ds(pl.multiple_of(j * TILE, TILE), TILE)
        b = br[:, c] + nn(act_f[...], wo[:, c])
        keep[0, :, c] = b[:rows]
        send[0, :, c] = b[rows:].astype(bf16)
        g = dn[:, c] + nn(dp[...], wi[:, c])
        keep[1, :, c] = g[:rows]
        send[1, :, c] = g[rows:].astype(bf16)

    lax.fori_loop(0, wi.shape[1] // TILE, back, None)


def grad_kernel(far, far2, wi, wo, gain, p, g, vwi, vwo, vp, vg, nb3, c3, act3, dp3, arrived, sent):
    rows = far.shape[0] // 2
    hid = wi.shape[0]
    loads = [
        pltpu.make_async_copy(src, dst, arrived.at[i])
        for i, (src, dst) in enumerate([(wi, vwi), (wo, vwo), (p, vp)])
    ]
    for load in loads:
        load.start()
    for k, half in enumerate((far, far2)):
        norm_into(half, 0, gain, nb3, k * rows, rows)
        c3[k * rows : (k + 1) * rows, :] = half[rows:, :]
    loads[0].wait()
    loads[1].wait()

    def hidden(j, _):
        h = pl.ds(pl.multiple_of(j * TILE, TILE), TILE)
        value, slope = gelu_both(nt(nb3[...], vwi[h, :]))
        act3[:, h] = value.astype(bf16)
        dp3[:, h] = (nt(c3[...], vwo[h, :]) * slope).astype(bf16)

    lax.fori_loop(0, hid // TILE, hidden, None)
    loads[2].wait()
    stores = []
    for k in range(FAR):
        c = slice(k * TILE, (k + 1) * TILE)
        gi = vp[c, :hid] + tn(nb3[:, c], dp3[...])
        vg[:, k, :, :hid] = gi.astype(bf16).reshape(NEAR, -1, hid)
        go = vp[c, hid:] + tn(c3[:, c], act3[...])
        vg[:, k, :, hid:] = go.astype(bf16).reshape(NEAR, -1, hid)
        store = pltpu.make_async_copy(vg.at[:, k], g.at[:, k], sent.at[k])
        store.start()
        stores.append(store)
    for store in stores:
        store.wait()


def sum_kernel(pieces, total):
    def step(k, _):
        total[k] = jnp.sum(pieces[:, k].astype(f32), axis=0).astype(bf16)

    lax.fori_loop(0, pieces.shape[1], step, None)


def last_kernel(pieces, g_in, g_out):
    hid = g_in.shape[1]
    total = jnp.sum(pieces[...].astype(f32), axis=0).astype(bf16)
    g_in[...] = total[:, :hid]
    g_out[...] = total[:, hid:]


def landed_kernel(a, b, c, d):
    c[0] = a[...]
    d[0] = b[...]


def local(kernel, outs, scratch, flops, moved, mib=62, **specs):
    return pl.pallas_call(
        kernel,
        out_shape=[jax.ShapeDtypeStruct(s, t) for s, t in outs],
        scratch_shapes=[pltpu.VMEM(*a) if isinstance(a, tuple) else a for a in scratch],
        compiler_params=pltpu.CompilerParams(vmem_limit_bytes=mib * 2**20),
        cost_estimate=pl.CostEstimate(flops=flops, bytes_accessed=moved, transcendentals=0),
        **specs,
    )


def layer(fwd_in, stash, cot, w_in, w_out, gain):
    xf, xb, ct = fwd_in[0], stash[0], cot[0]
    wi, wo = w_in[0], w_out[0]
    rows, dim = xf.shape
    hid = wi.shape[0]
    both = 2 * rows
    n_dp = lax.axis_size("dp")
    d = lax.axis_index("dp")
    part = hid // n_dp
    at = (d % NEAR * FAR + d // NEAR) * part
    mine = jnp.stack(
        [lax.dynamic_slice_in_dim(wi, at, part, 0), lax.dynamic_slice_in_dim(wo, at, part, 0)]
    )
    piece = to_chip(mine)
    far = to_chip(jnp.concatenate([xb, ct]))
    near = to_core(jnp.concatenate([xf, xb, ct]))
    nf, nb, c2, br, dn, p = local(
        own_kernel,
        [((both, dim), bf16)] * 3 + [((both, dim), f32)] * 2 + [((dim, 2 * hid), f32)],
        [((both, hid), bf16)] * 3,
        14 * both * hid * dim,
        11 * 2**20,
    )(xf, xb, ct, near, wi, wo, gain)
    col = gathered(piece, far_groups)
    whole = gathered(col, near_groups).reshape(n_dp, 2, part, dim)
    keep, send = local(
        rest_kernel,
        [((2, rows, dim), f32), ((2, rows, dim), bf16)],
        [((both, hid), bf16)] * 2 + [((hid, dim), bf16)] * 2,
        10 * both * hid * dim,
        8 * 2**20,
        mib=56,
    )(whole, nf, nb, c2, br, dn)
    sums = keep + to_core(send).astype(f32)
    out = (xf.astype(f32) + sums[0]).astype(bf16)
    passed_fwd = shifted(out, "section", 1)
    shard_x = xb.astype(f32)
    scale = scale_of(shard_x)
    push = sums[1] * gain
    mixed = jnp.mean(shard_x * push, axis=-1, keepdims=True)
    dx = ct.astype(f32) + scale * push - shard_x * scale * scale * scale * mixed
    passed_grad = shifted(dx.astype(bf16), "section", -1)
    far2 = to_core(far)
    cut = dim // n_dp
    (g,) = local(
        grad_kernel,
        [((NEAR, FAR, cut, 2 * hid), bf16)],
        [
            ((hid, dim), bf16),
            ((hid, dim), bf16),
            ((dim, 2 * hid), f32),
            ((NEAR, FAR, cut, 2 * hid), bf16),
            ((both, dim), bf16),
            ((both, dim), bf16),
            ((both, hid), bf16),
            ((both, hid), bf16),
            pltpu.SemaphoreType.DMA((3,)),
            pltpu.SemaphoreType.DMA((FAR,)),
        ],
        8 * both * hid * dim,
        9 * 2**20,
        mib=60,
        in_specs=[vmem, vmem, hbm, hbm, vmem, hbm],
        out_specs=[hbm],
    )(far, far2, wi, wo, gain, p)
    g = exchanged(g, near_groups)
    (g,) = local(sum_kernel, [(g.shape[1:], bf16)], [], 2**21, 2**21, mib=16)(g)
    g = exchanged(g, far_groups)
    passed_fwd, passed_grad = local(
        landed_kernel, [((1, rows, dim), bf16)] * 2, [], 2**20, 2**20, mib=16
    )(passed_fwd, passed_grad)
    g_in, g_out = local(last_kernel, [((cut, hid), bf16)] * 2, [], 2**18, 2**18, mib=16)(g)
    return passed_fwd, passed_grad, g_in.T[None], g_out.T[None]


def solution(mesh):
    in_specs = (
        P("section", ("dp", "mp"), None),
        P("section", ("dp", "mp"), None),
        P("section", ("dp", "mp"), None),
        P("section", "mp", None),
        P("section", "mp", None),
        P("section", None),
    )
    out_specs = (
        P("section", ("dp", "mp"), None),
        P("section", ("dp", "mp"), None),
        P("section", "mp", "dp"),
        P("section", "mp", "dp"),
    )
    return jax.shard_map(layer, mesh=mesh, in_specs=in_specs, out_specs=out_specs, check_vma=False)
```

```python
import functools

import jax
import jax.numpy as jnp
from jax import lax
from jax.experimental import pallas as pl
from jax.experimental.pallas import tpu as pltpu
from jax.sharding import PartitionSpec as P


norm_eps = 1e-05
gelu_coef = 0.7978845608


NEAR, FAR = 8, 4
near_groups = [[NEAR * k + j for j in range(NEAR)] for k in range(FAR)]
far_groups = [[NEAR * k + j for k in range(FAR)] for j in range(NEAR)]
other_chip = [(0, 2), (1, 3), (2, 0), (3, 1)]
other_core = [(0, 1), (1, 0), (2, 3), (3, 2)]

f32, bf16 = jnp.float32, jnp.bfloat16
vmem = pl.BlockSpec(memory_space=pltpu.VMEM)
hbm = pl.BlockSpec(memory_space=pltpu.HBM)
CHUNK = 16
EARLY = 16
TILE = 256


def to_chip(x):
    return lax.ppermute(x, "mp", other_chip)


def to_core(x):
    return lax.ppermute(x, "mp", other_core)


def shifted(x, axis, by):
    length = lax.axis_size(axis)
    return lax.ppermute(x, axis, [(i, (i + by) % length) for i in range(length)])


def gathered(x, groups, start=0, rows=None):
    n = len(groups[0])
    rows = rows or x.shape[-2]
    shape = (n, *x.shape[:-2], rows, x.shape[-1])
    (copies,) = pl.pallas_call(
        functools.partial(copies_kernel, start, rows),
        out_shape=[jax.ShapeDtypeStruct(shape, x.dtype)],
        in_specs=[vmem],
        out_specs=[hbm],
        scratch_shapes=[pltpu.SemaphoreType.DMA((n,))],
        compiler_params=pltpu.CompilerParams(vmem_limit_bytes=2 * 2**20),
        cost_estimate=pl.CostEstimate(flops=2**10, bytes_accessed=2**21, transcendentals=0),
    )(x)
    return lax.all_to_all(copies, "dp", 0, 0, tiled=True, axis_index_groups=groups)


def pack_kernel(part, wi, wo, xb, ct, mine, others, arrived):
    d = lax.axis_index("dp")
    at = pl.ds(pl.multiple_of((d % NEAR * FAR + d // NEAR) * part, part), part)
    later = xb.shape[0] - EARLY
    pairs = [
        (wi.at[at], mine.at[:part]),
        (wo.at[at], mine.at[part : 2 * part]),
        (xb.at[:EARLY], mine.at[2 * part : 2 * part + EARLY]),
        (ct.at[:EARLY], mine.at[2 * part + EARLY :]),
        (xb.at[EARLY:], others.at[:later]),
        (ct.at[EARLY:], others.at[later:]),
    ]
    copies = [pltpu.make_async_copy(a, b, arrived.at[i]) for i, (a, b) in enumerate(pairs)]
    for copy in copies:
        copy.start()
    for copy in copies:
        copy.wait()


def copies_kernel(start, rows, x, out, sent):
    source = x.at[start : start + rows] if len(x.shape) == 2 else x
    stores = [pltpu.make_async_copy(source, out.at[k], sent.at[k]) for k in range(out.shape[0])]
    for store in stores:
        store.start()
    for store in stores:
        store.wait()


def exchanged(x, groups):
    return lax.all_to_all(x, "dp", 0, 0, tiled=True, axis_index_groups=groups)


def gelu_both(v):
    t = jnp.tanh(gelu_coef * (v + 0.044715 * v * v * v))
    value = 0.5 * v * (1.0 + t)
    slope = 0.5 * (1.0 + t) + 0.5 * v * (1.0 - t * t) * gelu_coef * (1.0 + 0.134145 * v * v)
    return value, slope


def scale_of(xf):
    return lax.rsqrt(jnp.mean(xf * xf, axis=-1, keepdims=True) + norm_eps)


def nt(a, b):
    return lax.dot_general(a, b, (((1,), (1,)), ((), ())), preferred_element_type=f32)


def tn(a, b):
    return lax.dot_general(a, b, (((0,), (0,)), ((), ())), preferred_element_type=f32)


def nn(a, b):
    return jnp.dot(a, b, preferred_element_type=f32)


def norm_into(src, at, gain, dst, to, rows):
    def step(i, _):
        r = pl.multiple_of(i * CHUNK, CHUNK)
        x = src[pl.ds(at + r, CHUNK), :].astype(f32)
        dst[pl.ds(to + r, CHUNK), :] = (x * scale_of(x) * gain[...]).astype(bf16)

    lax.fori_loop(0, rows // CHUNK, step, None)


def own_kernel(
    xf, xb, ct, near, first, wi, wo, gain, nf, nb, c2, br, dn, p, vwi, vwo, vp, act_f, act, dp, arrived, sent
):
    rows = xf.shape[0]
    both = 2 * rows
    hid = wi.shape[0]
    loads = [
        pltpu.make_async_copy(wi, vwi, arrived.at[0]),
        pltpu.make_async_copy(wo, vwo, arrived.at[1]),
    ]
    for load in loads:
        load.start()
    norm_into(xb, 0, gain, nb, 0, rows)
    norm_into(near, rows, gain, nb, rows, rows)
    norm_into(first, 2 * EARLY, gain, nb, both, EARLY)
    norm_into(near, 3 * rows, gain, nb, both + EARLY, EARLY)
    norm_into(xf, 0, gain, nf, 0, rows)
    norm_into(near, 0, gain, nf, rows, rows)
    c2[:rows, :] = ct[...]
    c2[rows:both, :] = near[2 * rows : 3 * rows, :]
    c2[both : both + EARLY, :] = first[3 * EARLY :, :]
    c2[both + EARLY :, :] = near[3 * rows + EARLY :, :]
    for load in loads:
        load.wait()

    def hidden(j, _):
        h = pl.ds(pl.multiple_of(j * TILE, TILE), TILE)
        value, slope = gelu_both(nt(nb[...], vwi[h, :]))
        act[:, h] = value.astype(bf16)
        dp[:, h] = (nt(c2[...], vwo[h, :]) * slope).astype(bf16)
        value, _ = gelu_both(nt(nf[...], vwi[h, :]))
        act_f[:, h] = value.astype(bf16)

    lax.fori_loop(0, hid // TILE, hidden, None)
    stores = []
    for k in range(FAR):
        c = slice(k * TILE, (k + 1) * TILE)
        vp[c, :hid] = tn(nb[:, c], dp[...])
        vp[c, hid:] = tn(c2[:, c], act[...])
        store = pltpu.make_async_copy(vp.at[c], p.at[c], sent.at[k])
        store.start()
        stores.append(store)

    def back(j, _):
        c = pl.ds(pl.multiple_of(j * TILE, TILE), TILE)
        br[:, c] = nn(act_f[...], vwo[:, c])
        dn[:, c] = nn(dp[:both, :], vwi[:, c])

    lax.fori_loop(0, vwi.shape[1] // TILE, back, None)
    for store in stores:
        store.wait()


def rest_kernel(whole, nf, nb, c2, br, dn, keep, send, act_f, dp, wi, wo):
    rows = keep.shape[1]
    both = 2 * rows

    def split(i, _):
        r = pl.ds(pl.multiple_of(i * 16, 16), 16)
        wi[r, :] = whole[i, 0]
        wo[r, :] = whole[i, 1]

    lax.fori_loop(0, whole.shape[0], split, None)

    def hidden(j, _):
        h = pl.ds(pl.multiple_of(j * TILE, TILE), TILE)
        value, _ = gelu_both(nt(nf[...], wi[h, :]))
        act_f[:, h] = value.astype(bf16)
        _, slope = gelu_both(nt(nb[:both, :], wi[h, :]))
        dp[:, h] = (nt(c2[:both, :], wo[h, :]) * slope).astype(bf16)

    lax.fori_loop(0, wi.shape[0] // TILE, hidden, None)

    def back(j, _):
        c = pl.ds(pl.multiple_of(j * TILE, TILE), TILE)
        b = br[:, c] + nn(act_f[...], wo[:, c])
        keep[0, :, c] = b[:rows]
        send[0, :, c] = b[rows:].astype(bf16)
        g = dn[:, c] + nn(dp[...], wi[:, c])
        keep[1, :, c] = g[:rows]
        send[1, :, c] = g[rows:].astype(bf16)

    lax.fori_loop(0, wi.shape[1] // TILE, back, None)


def grad_kernel(far, far2, wi, wo, gain, p, g, vwi, vwo, vp, vg, nb3, c3, act3, dp3, arrived, sent):
    rows = far.shape[0] // 2
    hid = wi.shape[0]
    loads = [
        pltpu.make_async_copy(src, dst, arrived.at[i])
        for i, (src, dst) in enumerate([(wi, vwi), (wo, vwo), (p, vp)])
    ]
    for load in loads:
        load.start()
    for k, half in enumerate((far, far2)):
        norm_into(half, 0, gain, nb3, k * rows, rows)
        c3[k * rows : (k + 1) * rows, :] = half[rows:, :]
    loads[0].wait()
    loads[1].wait()

    def hidden(j, _):
        h = pl.ds(pl.multiple_of(j * TILE, TILE), TILE)
        value, slope = gelu_both(nt(nb3[...], vwi[h, :]))
        act3[:, h] = value.astype(bf16)
        dp3[:, h] = (nt(c3[...], vwo[h, :]) * slope).astype(bf16)

    lax.fori_loop(0, hid // TILE, hidden, None)
    loads[2].wait()
    stores = []
    for k in range(FAR):
        c = slice(k * TILE, (k + 1) * TILE)
        gi = vp[c, :hid] + tn(nb3[:, c], dp3[...])
        vg[:, k, :, :hid] = gi.astype(bf16).reshape(NEAR, -1, hid)
        go = vp[c, hid:] + tn(c3[:, c], act3[...])
        vg[:, k, :, hid:] = go.astype(bf16).reshape(NEAR, -1, hid)
        store = pltpu.make_async_copy(vg.at[:, k], g.at[:, k], sent.at[k])
        store.start()
        stores.append(store)
    for store in stores:
        store.wait()


def sum_kernel(pieces, total):
    def step(k, _):
        total[k] = jnp.sum(pieces[:, k].astype(f32), axis=0).astype(bf16)

    lax.fori_loop(0, pieces.shape[1], step, None)


def last_kernel(pieces, g_in, g_out):
    hid = g_in.shape[1]
    total = jnp.sum(pieces[...].astype(f32), axis=0).astype(bf16)
    g_in[...] = total[:, :hid]
    g_out[...] = total[:, hid:]


def landed_kernel(a, b, c, d):
    c[0] = a[...]
    d[0] = b[...]


def local(kernel, outs, scratch, flops, moved, mib=62, **specs):
    return pl.pallas_call(
        kernel,
        out_shape=[jax.ShapeDtypeStruct(s, t) for s, t in outs],
        scratch_shapes=[pltpu.VMEM(*a) if isinstance(a, tuple) else a for a in scratch],
        compiler_params=pltpu.CompilerParams(vmem_limit_bytes=mib * 2**20),
        cost_estimate=pl.CostEstimate(flops=flops, bytes_accessed=moved, transcendentals=0),
        **specs,
    )


def layer(fwd_in, stash, cot, w_in, w_out, gain):
    xf, xb, ct = fwd_in[0], stash[0], cot[0]
    wi, wo = w_in[0], w_out[0]
    rows, dim = xf.shape
    hid = wi.shape[0]
    both = 2 * rows
    n_dp = lax.axis_size("dp")
    part = hid // n_dp
    mine, others = pl.pallas_call(
        functools.partial(pack_kernel, part),
        out_shape=[
            jax.ShapeDtypeStruct((2 * part + 2 * EARLY, dim), bf16),
            jax.ShapeDtypeStruct((2 * (rows - EARLY), dim), bf16),
        ],
        in_specs=[hbm] * 4,
        out_specs=[vmem] * 2,
        scratch_shapes=[pltpu.SemaphoreType.DMA((6,))],
        compiler_params=pltpu.CompilerParams(vmem_limit_bytes=62 * 2**20),
        cost_estimate=pl.CostEstimate(flops=2**10, bytes_accessed=2**20, transcendentals=0),
    )(wi, wo, xb, ct)
    first = to_chip(mine)
    far = to_chip(others)
    near = to_core(jnp.concatenate([xf, xb, ct, first[2 * part :]]))
    more = both + 2 * EARLY
    nf, nb, c2, br, dn, p = local(
        own_kernel,
        [((both, dim), bf16)]
        + [((more, dim), bf16)] * 2
        + [((both, dim), f32)] * 2
        + [((dim, 2 * hid), f32)],
        [
            ((hid, dim), bf16),
            ((hid, dim), bf16),
            ((dim, 2 * hid), f32),
            ((both, hid), bf16),
            ((more, hid), bf16),
            ((more, hid), bf16),
            pltpu.SemaphoreType.DMA((2,)),
            pltpu.SemaphoreType.DMA((FAR,)),
        ],
        14 * both * hid * dim,
        11 * 2**20,
        in_specs=[vmem] * 5 + [hbm, hbm, vmem],
        out_specs=[vmem] * 5 + [hbm],
    )(xf, xb, ct, near, first, wi, wo, gain)
    col = gathered(first, far_groups, 0, 2 * part)
    whole = gathered(col, near_groups).reshape(n_dp, 2, part, dim)
    keep, send = local(
        rest_kernel,
        [((2, rows, dim), f32), ((2, rows, dim), bf16)],
        [((both, hid), bf16)] * 2 + [((hid, dim), bf16)] * 2,
        10 * both * hid * dim,
        8 * 2**20,
        mib=56,
    )(whole, nf, nb, c2, br, dn)
    sums = keep + to_core(send).astype(f32)
    out = (xf.astype(f32) + sums[0]).astype(bf16)
    passed_fwd = shifted(out, "section", 1)
    shard_x = xb.astype(f32)
    scale = scale_of(shard_x)
    push = sums[1] * gain
    mixed = jnp.mean(shard_x * push, axis=-1, keepdims=True)
    dx = ct.astype(f32) + scale * push - shard_x * scale * scale * scale * mixed
    passed_grad = shifted(dx.astype(bf16), "section", -1)
    far2 = to_core(far)
    cut = dim // n_dp
    (g,) = local(
        grad_kernel,
        [((NEAR, FAR, cut, 2 * hid), bf16)],
        [
            ((hid, dim), bf16),
            ((hid, dim), bf16),
            ((dim, 2 * hid), f32),
            ((NEAR, FAR, cut, 2 * hid), bf16),
            ((both - 2 * EARLY, dim), bf16),
            ((both - 2 * EARLY, dim), bf16),
            ((both - 2 * EARLY, hid), bf16),
            ((both - 2 * EARLY, hid), bf16),
            pltpu.SemaphoreType.DMA((3,)),
            pltpu.SemaphoreType.DMA((FAR,)),
        ],
        8 * both * hid * dim,
        9 * 2**20,
        mib=60,
        in_specs=[vmem, vmem, hbm, hbm, vmem, hbm],
        out_specs=[hbm],
    )(far, far2, wi, wo, gain, p)
    g = exchanged(g, near_groups)
    (g,) = local(sum_kernel, [(g.shape[1:], bf16)], [], 2**21, 2**21, mib=16)(g)
    g = exchanged(g, far_groups)
    passed_fwd, passed_grad = local(
        landed_kernel, [((1, rows, dim), bf16)] * 2, [], 2**20, 2**20, mib=16
    )(passed_fwd, passed_grad)
    g_in, g_out = local(last_kernel, [((cut, hid), bf16)] * 2, [], 2**18, 2**18, mib=16)(g)
    return passed_fwd, passed_grad, g_in.T[None], g_out.T[None]


def solution(mesh):
    in_specs = (
        P("section", ("dp", "mp"), None),
        P("section", ("dp", "mp"), None),
        P("section", ("dp", "mp"), None),
        P("section", "mp", None),
        P("section", "mp", None),
        P("section", None),
    )
    out_specs = (
        P("section", ("dp", "mp"), None),
        P("section", ("dp", "mp"), None),
        P("section", "mp", "dp"),
        P("section", "mp", "dp"),
    )
    return jax.shard_map(layer, mesh=mesh, in_specs=in_specs, out_specs=out_specs, check_vma=False)
```

```python
import jax
import jax.numpy as jnp
from jax import lax
from jax.experimental import pallas as pl
from jax.experimental.pallas import tpu as pltpu
from jax.sharding import PartitionSpec as P


norm_eps = 1e-05
gelu_coef = 0.7978845608


NEAR, FAR = 8, 4
near_groups = [[NEAR * k + j for j in range(NEAR)] for k in range(FAR)]
far_groups = [[NEAR * k + j for k in range(FAR)] for j in range(NEAR)]
other_chip = [(0, 2), (1, 3), (2, 0), (3, 1)]
other_core = [(0, 1), (1, 0), (2, 3), (3, 2)]

f32, bf16 = jnp.float32, jnp.bfloat16
vmem = pl.BlockSpec(memory_space=pltpu.VMEM)
hbm = pl.BlockSpec(memory_space=pltpu.HBM)
CHUNK = 32
TILE = 256


def to_chip(x):
    return lax.ppermute(x, "mp", other_chip)


def to_core(x):
    return lax.ppermute(x, "mp", other_core)


def shifted(x, axis, by):
    length = lax.axis_size(axis)
    return lax.ppermute(x, axis, [(i, (i + by) % length) for i in range(length)])


def gathered(x, groups):
    copies = jnp.broadcast_to(x, (len(groups[0]), *x.shape))
    return lax.all_to_all(copies, "dp", 0, 0, tiled=True, axis_index_groups=groups)


def exchanged(x, groups):
    return lax.all_to_all(x, "dp", 0, 0, tiled=True, axis_index_groups=groups)


def gelu_both(v):
    t = jnp.tanh(gelu_coef * (v + 0.044715 * v * v * v))
    value = 0.5 * v * (1.0 + t)
    slope = 0.5 * (1.0 + t) + 0.5 * v * (1.0 - t * t) * gelu_coef * (1.0 + 0.134145 * v * v)
    return value, slope


def scale_of(xf):
    return lax.rsqrt(jnp.mean(xf * xf, axis=-1, keepdims=True) + norm_eps)


def nt(a, b):
    return lax.dot_general(a, b, (((1,), (1,)), ((), ())), preferred_element_type=f32)


def tn(a, b):
    return lax.dot_general(a, b, (((0,), (0,)), ((), ())), preferred_element_type=f32)


def nn(a, b):
    return jnp.dot(a, b, preferred_element_type=f32)


def norm_into(src, at, gain, dst, to, rows):
    def step(i, _):
        r = pl.multiple_of(i * CHUNK, CHUNK)
        x = src[pl.ds(at + r, CHUNK), :].astype(f32)
        dst[pl.ds(to + r, CHUNK), :] = (x * scale_of(x) * gain[...]).astype(bf16)

    lax.fori_loop(0, rows // CHUNK, step, None)


def own_kernel(xf, xb, ct, near, wi, wo, gain, nf, nb, c2, br, dn, p, act_f, act, dp):
    rows = xf.shape[0]
    hid = wi.shape[0]
    norm_into(xf, 0, gain, nf, 0, rows)
    norm_into(near, 0, gain, nf, rows, rows)
    norm_into(xb, 0, gain, nb, 0, rows)
    norm_into(near, rows, gain, nb, rows, rows)
    c2[:rows, :] = ct[...]
    c2[rows:, :] = near[2 * rows :, :]

    def hidden(j, _):
        h = pl.ds(pl.multiple_of(j * TILE, TILE), TILE)
        value, _ = gelu_both(nt(nf[...], wi[h, :]))
        act_f[:, h] = value.astype(bf16)
        value, slope = gelu_both(nt(nb[...], wi[h, :]))
        act[:, h] = value.astype(bf16)
        dp[:, h] = (nt(c2[...], wo[h, :]) * slope).astype(bf16)

    lax.fori_loop(0, wi.shape[0] // TILE, hidden, None)

    def back(j, _):
        c = pl.ds(pl.multiple_of(j * TILE, TILE), TILE)
        br[:, c] = nn(act_f[...], wo[:, c])
        dn[:, c] = nn(dp[...], wi[:, c])
        p[c, :hid] = tn(nb[:, c], dp[...])
        p[c, hid:] = tn(c2[:, c], act[...])

    lax.fori_loop(0, wi.shape[1] // TILE, back, None)


def rest_kernel(whole, nf, nb, c2, br, dn, keep, send, act_f, dp, wi, wo):
    rows = keep.shape[1]

    def split(i, _):
        r = pl.ds(pl.multiple_of(i * 16, 16), 16)
        wi[r, :] = whole[i, 0]
        wo[r, :] = whole[i, 1]

    lax.fori_loop(0, whole.shape[0], split, None)

    def hidden(j, _):
        h = pl.ds(pl.multiple_of(j * TILE, TILE), TILE)
        value, _ = gelu_both(nt(nf[...], wi[h, :]))
        act_f[:, h] = value.astype(bf16)
        _, slope = gelu_both(nt(nb[...], wi[h, :]))
        dp[:, h] = (nt(c2[...], wo[h, :]) * slope).astype(bf16)

    lax.fori_loop(0, wi.shape[0] // TILE, hidden, None)

    def back(j, _):
        c = pl.ds(pl.multiple_of(j * TILE, TILE), TILE)
        b = br[:, c] + nn(act_f[...], wo[:, c])
        keep[0, :, c] = b[:rows]
        send[0, :, c] = b[rows:].astype(bf16)
        g = dn[:, c] + nn(dp[...], wi[:, c])
        keep[1, :, c] = g[:rows]
        send[1, :, c] = g[rows:].astype(bf16)

    lax.fori_loop(0, wi.shape[1] // TILE, back, None)


def half_kernel(far, far2, wi, gain, nbt, act, slope, nb):
    rows = far.shape[0]
    for k, part in enumerate((far, far2)):
        norm_into(part, 0, gain, nb, k * rows, rows)

    def hidden(j, _):
        h = pl.ds(pl.multiple_of(j * TILE, TILE), TILE)
        value, down = gelu_both(nt(nb[...], wi[h, :]))
        act[:, h] = value.astype(bf16)
        slope[:, h] = down
        for k in range(2):
            c = pl.ds(pl.multiple_of((2 * j + k) * TILE, TILE), TILE)
            nbt[c, :] = nb[:, c].T

    lax.fori_loop(0, wi.shape[0] // TILE, hidden, None)


def grad_kernel(far, far2, wo, nbt, act, slope, p, g, vwo, vnbt, vact, vslope, vp, vg, c3, dp3, arrived, sent):
    rows = far.shape[0]
    hid = wo.shape[0]
    pairs = [(wo, vwo), (slope, vslope), (nbt, vnbt), (act, vact), (p, vp)]
    loads = [pltpu.make_async_copy(a, b, arrived.at[i]) for i, (a, b) in enumerate(pairs)]
    for load in loads:
        load.start()
    c3[:rows, :] = far[...]
    c3[rows:, :] = far2[...]
    loads[0].wait()
    loads[1].wait()

    def hidden(j, _):
        h = pl.ds(pl.multiple_of(j * TILE, TILE), TILE)
        dp3[:, h] = (nt(c3[...], vwo[h, :]) * vslope[:, h]).astype(bf16)

    lax.fori_loop(0, hid // TILE, hidden, None)
    for load in loads[2:]:
        load.wait()
    stores = []
    for k in range(FAR):
        c = slice(k * TILE, (k + 1) * TILE)
        gi = vp[c, :hid] + nn(vnbt[c, :], dp3[...])
        vg[:, k, :, :hid] = gi.astype(bf16).reshape(NEAR, -1, hid)
        go = vp[c, hid:] + tn(c3[:, c], vact[...])
        vg[:, k, :, hid:] = go.astype(bf16).reshape(NEAR, -1, hid)
        store = pltpu.make_async_copy(vg.at[:, k], g.at[:, k], sent.at[k])
        store.start()
        stores.append(store)
    for store in stores:
        store.wait()


def sum_kernel(pieces, total):
    def step(k, _):
        total[k] = jnp.sum(pieces[:, k].astype(f32), axis=0).astype(bf16)

    lax.fori_loop(0, pieces.shape[1], step, None)


def last_kernel(pieces, g_in, g_out):
    hid = g_in.shape[1]
    total = jnp.sum(pieces[...].astype(f32), axis=0).astype(bf16)
    g_in[...] = total[:, :hid]
    g_out[...] = total[:, hid:]


def landed_kernel(a, b, c, d):
    c[0] = a[...]
    d[0] = b[...]


def local(kernel, outs, scratch, flops, moved, mib=62, **specs):
    return pl.pallas_call(
        kernel,
        out_shape=[jax.ShapeDtypeStruct(s, t) for s, t in outs],
        scratch_shapes=[pltpu.VMEM(*a) if isinstance(a, tuple) else a for a in scratch],
        compiler_params=pltpu.CompilerParams(vmem_limit_bytes=mib * 2**20),
        cost_estimate=pl.CostEstimate(flops=flops, bytes_accessed=moved, transcendentals=0),
        **specs,
    )


def layer(fwd_in, stash, cot, w_in, w_out, gain):
    xf, xb, ct = fwd_in[0], stash[0], cot[0]
    wi, wo = w_in[0], w_out[0]
    rows, dim = xf.shape
    hid = wi.shape[0]
    both = 2 * rows
    n_dp = lax.axis_size("dp")
    d = lax.axis_index("dp")
    part = hid // n_dp
    at = (d % NEAR * FAR + d // NEAR) * part
    mine = jnp.stack(
        [lax.dynamic_slice_in_dim(wi, at, part, 0), lax.dynamic_slice_in_dim(wo, at, part, 0)]
    )
    piece = to_chip(mine)
    far_s = to_chip(xb)
    far_c = to_chip(ct)
    near = to_core(jnp.concatenate([xf, xb, ct]))
    nf, nb, c2, br, dn, p = local(
        own_kernel,
        [((both, dim), bf16)] * 3 + [((both, dim), f32)] * 2 + [((dim, 2 * hid), f32)],
        [((both, hid), bf16)] * 3,
        14 * both * hid * dim,
        11 * 2**20,
    )(xf, xb, ct, near, wi, wo, gain)
    col = gathered(piece, far_groups)
    whole = gathered(col, near_groups).reshape(n_dp, 2, part, dim)
    keep, send = local(
        rest_kernel,
        [((2, rows, dim), f32), ((2, rows, dim), bf16)],
        [((both, hid), bf16)] * 2 + [((hid, dim), bf16)] * 2,
        10 * both * hid * dim,
        8 * 2**20,
        mib=56,
    )(whole, nf, nb, c2, br, dn)
    sums = keep + to_core(send).astype(f32)
    out = (xf.astype(f32) + sums[0]).astype(bf16)
    passed_fwd = shifted(out, "section", 1)
    shard_x = xb.astype(f32)
    scale = scale_of(shard_x)
    push = sums[1] * gain
    mixed = jnp.mean(shard_x * push, axis=-1, keepdims=True)
    dx = ct.astype(f32) + scale * push - shard_x * scale * scale * scale * mixed
    passed_grad = shifted(dx.astype(bf16), "section", -1)
    far_s2 = to_core(far_s)
    nbt3, act3, slope3 = local(
        half_kernel,
        [((dim, both), bf16), ((both, hid), bf16), ((both, hid), f32)],
        [((both, dim), bf16)],
        2 * both * hid * dim,
        4 * 2**20,
    )(far_s, far_s2, wi, gain)
    far_c2 = to_core(far_c)
    cut = dim // n_dp
    (g,) = local(
        grad_kernel,
        [((NEAR, FAR, cut, 2 * hid), bf16)],
        [
            ((hid, dim), bf16),
            ((dim, both), bf16),
            ((both, hid), bf16),
            ((both, hid), f32),
            ((dim, 2 * hid), f32),
            ((NEAR, FAR, cut, 2 * hid), bf16),
            ((both, dim), bf16),
            ((both, hid), bf16),
            pltpu.SemaphoreType.DMA((5,)),
            pltpu.SemaphoreType.DMA((FAR,)),
        ],
        6 * both * hid * dim,
        9 * 2**20,
        in_specs=[vmem, vmem, hbm, hbm, hbm, hbm, hbm],
        out_specs=[hbm],
    )(far_c, far_c2, wo, nbt3, act3, slope3, p)
    g = exchanged(g, near_groups)
    (g,) = local(sum_kernel, [(g.shape[1:], bf16)], [], 2**21, 2**21, mib=16)(g)
    g = exchanged(g, far_groups)
    passed_fwd, passed_grad = local(
        landed_kernel, [((1, rows, dim), bf16)] * 2, [], 2**20, 2**20, mib=16
    )(passed_fwd, passed_grad)
    g_in, g_out = local(last_kernel, [((cut, hid), bf16)] * 2, [], 2**18, 2**18, mib=16)(g)
    return passed_fwd, passed_grad, g_in.T[None], g_out.T[None]


def solution(mesh):
    in_specs = (
        P("section", ("dp", "mp"), None),
        P("section", ("dp", "mp"), None),
        P("section", ("dp", "mp"), None),
        P("section", "mp", None),
        P("section", "mp", None),
        P("section", None),
    )
    out_specs = (
        P("section", ("dp", "mp"), None),
        P("section", ("dp", "mp"), None),
        P("section", "mp", "dp"),
        P("section", "mp", "dp"),
    )
    return jax.shard_map(layer, mesh=mesh, in_specs=in_specs, out_specs=out_specs, check_vma=False)
```

```python
import jax
import jax.numpy as jnp
from jax import lax
from jax.experimental import pallas as pl
from jax.experimental.pallas import tpu as pltpu
from jax.sharding import PartitionSpec as P


norm_eps = 1e-05
gelu_coef = 0.7978845608


NEAR, FAR = 8, 4
near_groups = [[NEAR * k + j for j in range(NEAR)] for k in range(FAR)]
far_groups = [[NEAR * k + j for k in range(FAR)] for j in range(NEAR)]
other_chip = [(0, 2), (1, 3), (2, 0), (3, 1)]
other_core = [(0, 1), (1, 0), (2, 3), (3, 2)]

f32, bf16 = jnp.float32, jnp.bfloat16
vmem = pl.BlockSpec(memory_space=pltpu.VMEM)
hbm = pl.BlockSpec(memory_space=pltpu.HBM)
CHUNK = 32
TILE = 256


def to_chip(x):
    return lax.ppermute(x, "mp", other_chip)


def to_core(x):
    return lax.ppermute(x, "mp", other_core)


def shifted(x, axis, by):
    length = lax.axis_size(axis)
    return lax.ppermute(x, axis, [(i, (i + by) % length) for i in range(length)])


def gathered(x, groups):
    copies = jnp.broadcast_to(x, (len(groups[0]), *x.shape))
    return lax.all_to_all(copies, "dp", 0, 0, tiled=True, axis_index_groups=groups)


def exchanged(x, groups):
    return lax.all_to_all(x, "dp", 0, 0, tiled=True, axis_index_groups=groups)


def gelu_both(v):
    t = jnp.tanh(gelu_coef * (v + 0.044715 * v * v * v))
    value = 0.5 * v * (1.0 + t)
    slope = 0.5 * (1.0 + t) + 0.5 * v * (1.0 - t * t) * gelu_coef * (1.0 + 0.134145 * v * v)
    return value, slope


def scale_of(xf):
    return lax.rsqrt(jnp.mean(xf * xf, axis=-1, keepdims=True) + norm_eps)


def nt(a, b):
    return lax.dot_general(a, b, (((1,), (1,)), ((), ())), preferred_element_type=f32)


def tn(a, b):
    return lax.dot_general(a, b, (((0,), (0,)), ((), ())), preferred_element_type=f32)


def nn(a, b):
    return jnp.dot(a, b, preferred_element_type=f32)


def norm_into(src, at, gain, dst, to, rows):
    for r in range(0, rows, CHUNK):
        x = src[at + r : at + r + CHUNK, :].astype(f32)
        dst[to + r : to + r + CHUNK, :] = (x * scale_of(x) * gain[...]).astype(bf16)


def own_kernel(xb, ct, near, wi, wo, gain, nb, c2, dp, p, vwi, vwo, vp, act, arrived, sent):
    rows = xb.shape[0]
    hid = wi.shape[0]
    loads = [
        pltpu.make_async_copy(wi, vwi, arrived.at[0]),
        pltpu.make_async_copy(wo, vwo, arrived.at[1]),
    ]
    for load in loads:
        load.start()
    norm_into(xb, 0, gain, nb, 0, rows)
    norm_into(near, rows, gain, nb, rows, rows)
    c2[:rows, :] = ct[...]
    c2[rows:, :] = near[2 * rows :, :]
    for load in loads:
        load.wait()

    def hidden(j, _):
        h = pl.ds(pl.multiple_of(j * TILE, TILE), TILE)
        value, slope = gelu_both(nt(nb[...], vwi[h, :]))
        act[:, h] = value.astype(bf16)
        dp[:, h] = (nt(c2[...], vwo[h, :]) * slope).astype(bf16)

    lax.fori_loop(0, hid // TILE, hidden, None)
    stores = []
    for k in range(FAR):
        c = slice(k * TILE, (k + 1) * TILE)
        vp[c, :hid] = tn(nb[:, c], dp[...])
        vp[c, hid:] = tn(c2[:, c], act[...])
        store = pltpu.make_async_copy(vp.at[c], p.at[c], sent.at[k])
        store.start()
        stores.append(store)
    for store in stores:
        store.wait()


def forward_kernel(xf, near, wi, wo, gain, nf, br, act):
    rows = xf.shape[0]
    norm_into(xf, 0, gain, nf, 0, rows)
    norm_into(near, 0, gain, nf, rows, rows)

    def hidden(j, _):
        h = pl.ds(pl.multiple_of(j * TILE, TILE), TILE)
        value, _ = gelu_both(nt(nf[...], wi[h, :]))
        act[:, h] = value.astype(bf16)

    lax.fori_loop(0, wi.shape[0] // TILE, hidden, None)
    times_kernel(act, wo, br)


def times_kernel(a, w, total):
    def back(j, _):
        c = pl.ds(pl.multiple_of(j * TILE, TILE), TILE)
        total[:, c] = nn(a[...], w[:, c])

    lax.fori_loop(0, w.shape[1] // TILE, back, None)


def rest_kernel(whole, nf, nb, c2, br, dn, keep, send, act_f, dp, wi, wo):
    rows = keep.shape[1]

    def split(i, _):
        r = pl.ds(pl.multiple_of(i * 16, 16), 16)
        wi[r, :] = whole[i, 0]
        wo[r, :] = whole[i, 1]

    lax.fori_loop(0, whole.shape[0], split, None)

    def hidden(j, _):
        h = pl.ds(pl.multiple_of(j * TILE, TILE), TILE)
        value, _ = gelu_both(nt(nf[...], wi[h, :]))
        act_f[:, h] = value.astype(bf16)
        _, slope = gelu_both(nt(nb[...], wi[h, :]))
        dp[:, h] = (nt(c2[...], wo[h, :]) * slope).astype(bf16)

    lax.fori_loop(0, wi.shape[0] // TILE, hidden, None)

    def back(j, _):
        c = pl.ds(pl.multiple_of(j * TILE, TILE), TILE)
        b = br[:, c] + nn(act_f[...], wo[:, c])
        keep[0, :, c] = b[:rows]
        send[0, :, c] = b[rows:].astype(bf16)
        g = dn[:, c] + nn(dp[...], wi[:, c])
        keep[1, :, c] = g[:rows]
        send[1, :, c] = g[rows:].astype(bf16)

    lax.fori_loop(0, wi.shape[1] // TILE, back, None)


def half_kernel(far, far2, wi, gain, nbt, act, slope, nb):
    rows = far.shape[0]
    for k, part in enumerate((far, far2)):
        norm_into(part, 0, gain, nb, k * rows, rows)

    def hidden(j, _):
        h = pl.ds(pl.multiple_of(j * TILE, TILE), TILE)
        value, down = gelu_both(nt(nb[...], wi[h, :]))
        act[:, h] = value.astype(bf16)
        slope[:, h] = down
        for k in range(2):
            c = pl.ds(pl.multiple_of((2 * j + k) * TILE, TILE), TILE)
            nbt[c, :] = nb[:, c].T

    lax.fori_loop(0, wi.shape[0] // TILE, hidden, None)


def grad_kernel(far, far2, wo, nbt, act, slope, p, g, vwo, vnbt, vact, vslope, vp, vg, c3, dp3, arrived, sent):
    rows = far.shape[0]
    hid = wo.shape[0]
    pairs = [(wo, vwo), (slope, vslope), (nbt, vnbt), (act, vact), (p, vp)]
    loads = [pltpu.make_async_copy(a, b, arrived.at[i]) for i, (a, b) in enumerate(pairs)]
    for load in loads:
        load.start()
    c3[:rows, :] = far[...]
    c3[rows:, :] = far2[...]
    loads[0].wait()
    loads[1].wait()

    def hidden(j, _):
        h = pl.ds(pl.multiple_of(j * TILE, TILE), TILE)
        dp3[:, h] = (nt(c3[...], vwo[h, :]) * vslope[:, h]).astype(bf16)

    lax.fori_loop(0, hid // TILE, hidden, None)
    for load in loads[2:]:
        load.wait()
    stores = []
    for k in range(FAR):
        c = slice(k * TILE, (k + 1) * TILE)
        gi = vp[c, :hid] + nn(vnbt[c, :], dp3[...])
        vg[:, k, :, :hid] = gi.astype(bf16).reshape(NEAR, -1, hid)
        go = vp[c, hid:] + tn(c3[:, c], vact[...])
        vg[:, k, :, hid:] = go.astype(bf16).reshape(NEAR, -1, hid)
        store = pltpu.make_async_copy(vg.at[:, k], g.at[:, k], sent.at[k])
        store.start()
        stores.append(store)
    for store in stores:
        store.wait()


def sum_kernel(pieces, total):
    def step(k, _):
        total[k] = jnp.sum(pieces[:, k].astype(f32), axis=0).astype(bf16)

    lax.fori_loop(0, pieces.shape[1], step, None)


def last_kernel(pieces, g_in, g_out):
    hid = g_in.shape[1]
    total = jnp.sum(pieces[...].astype(f32), axis=0).astype(bf16)
    g_in[...] = total[:, :hid]
    g_out[...] = total[:, hid:]


def landed_kernel(a, b, c, d):
    c[0] = a[...]
    d[0] = b[...]


def local(kernel, outs, scratch, flops, moved, mib=62, **specs):
    return pl.pallas_call(
        kernel,
        out_shape=[jax.ShapeDtypeStruct(s, t) for s, t in outs],
        scratch_shapes=[pltpu.VMEM(*a) if isinstance(a, tuple) else a for a in scratch],
        compiler_params=pltpu.CompilerParams(vmem_limit_bytes=mib * 2**20),
        cost_estimate=pl.CostEstimate(flops=flops, bytes_accessed=moved, transcendentals=0),
        **specs,
    )


def layer(fwd_in, stash, cot, w_in, w_out, gain):
    xf, xb, ct = fwd_in[0], stash[0], cot[0]
    wi, wo = w_in[0], w_out[0]
    rows, dim = xf.shape
    hid = wi.shape[0]
    both = 2 * rows
    n_dp = lax.axis_size("dp")
    d = lax.axis_index("dp")
    part = hid // n_dp
    at = (d % NEAR * FAR + d // NEAR) * part
    mine = jnp.stack(
        [lax.dynamic_slice_in_dim(wi, at, part, 0), lax.dynamic_slice_in_dim(wo, at, part, 0)]
    )
    piece = to_chip(mine)
    far_s = to_chip(xb)
    far_c = to_chip(ct)
    near = to_core(jnp.concatenate([xf, xb, ct]))
    nb, c2, dp, p = local(
        own_kernel,
        [((both, dim), bf16)] * 2 + [((both, hid), bf16), ((dim, 2 * hid), f32)],
        [
            ((hid, dim), bf16),
            ((hid, dim), bf16),
            ((dim, 2 * hid), f32),
            ((both, hid), bf16),
            pltpu.SemaphoreType.DMA((2,)),
            pltpu.SemaphoreType.DMA((FAR,)),
        ],
        8 * both * hid * dim,
        9 * 2**20,
        in_specs=[vmem] * 3 + [hbm, hbm, vmem],
        out_specs=[vmem] * 3 + [hbm],
    )(xb, ct, near, wi, wo, gain)
    nf, br = local(
        forward_kernel,
        [((both, dim), bf16), ((both, dim), f32)],
        [((both, hid), bf16)],
        4 * both * hid * dim,
        4 * 2**20,
    )(xf, near, wi, wo, gain)
    (dn,) = local(times_kernel, [((both, dim), f32)], [], 2 * both * hid * dim, 2**21)(dp, wi)
    col = gathered(piece, far_groups)
    whole = gathered(col, near_groups).reshape(n_dp, 2, part, dim)
    keep, send = local(
        rest_kernel,
        [((2, rows, dim), f32), ((2, rows, dim), bf16)],
        [((both, hid), bf16)] * 2 + [((hid, dim), bf16)] * 2,
        10 * both * hid * dim,
        8 * 2**20,
        mib=56,
    )(whole, nf, nb, c2, br, dn)
    sums = keep + to_core(send).astype(f32)
    out = (xf.astype(f32) + sums[0]).astype(bf16)
    passed_fwd = shifted(out, "section", 1)
    shard_x = xb.astype(f32)
    scale = scale_of(shard_x)
    push = sums[1] * gain
    mixed = jnp.mean(shard_x * push, axis=-1, keepdims=True)
    dx = ct.astype(f32) + scale * push - shard_x * scale * scale * scale * mixed
    passed_grad = shifted(dx.astype(bf16), "section", -1)
    far_s2 = to_core(far_s)
    nbt3, act3, slope3 = local(
        half_kernel,
        [((dim, both), bf16), ((both, hid), bf16), ((both, hid), f32)],
        [((both, dim), bf16)],
        2 * both * hid * dim,
        4 * 2**20,
    )(far_s, far_s2, wi, gain)
    far_c2 = to_core(far_c)
    cut = dim // n_dp
    (g,) = local(
        grad_kernel,
        [((NEAR, FAR, cut, 2 * hid), bf16)],
        [
            ((hid, dim), bf16),
            ((dim, both), bf16),
            ((both, hid), bf16),
            ((both, hid), f32),
            ((dim, 2 * hid), f32),
            ((NEAR, FAR, cut, 2 * hid), bf16),
            ((both, dim), bf16),
            ((both, hid), bf16),
            pltpu.SemaphoreType.DMA((5,)),
            pltpu.SemaphoreType.DMA((FAR,)),
        ],
        6 * both * hid * dim,
        9 * 2**20,
        in_specs=[vmem, vmem, hbm, hbm, hbm, hbm, hbm],
        out_specs=[hbm],
    )(far_c, far_c2, wo, nbt3, act3, slope3, p)
    g = exchanged(g, near_groups)
    (g,) = local(sum_kernel, [(g.shape[1:], bf16)], [], 2**21, 2**21, mib=16)(g)
    g = exchanged(g, far_groups)
    passed_fwd, passed_grad = local(
        landed_kernel, [((1, rows, dim), bf16)] * 2, [], 2**20, 2**20, mib=16
    )(passed_fwd, passed_grad)
    g_in, g_out = local(last_kernel, [((cut, hid), bf16)] * 2, [], 2**18, 2**18, mib=16)(g)
    return passed_fwd, passed_grad, g_in.T[None], g_out.T[None]


def solution(mesh):
    in_specs = (
        P("section", ("dp", "mp"), None),
        P("section", ("dp", "mp"), None),
        P("section", ("dp", "mp"), None),
        P("section", "mp", None),
        P("section", "mp", None),
        P("section", None),
    )
    out_specs = (
        P("section", ("dp", "mp"), None),
        P("section", ("dp", "mp"), None),
        P("section", "mp", "dp"),
        P("section", "mp", "dp"),
    )
    return jax.shard_map(layer, mesh=mesh, in_specs=in_specs, out_specs=out_specs, check_vma=False)
```

```python
import jax
import jax.numpy as jnp
from jax import lax
from jax.experimental import pallas as pl
from jax.experimental.pallas import tpu as pltpu
from jax.sharding import PartitionSpec as P


norm_eps = 1e-05
gelu_coef = 0.7978845608


NEAR, FAR = 8, 4
near_groups = [[NEAR * k + j for j in range(NEAR)] for k in range(FAR)]
far_groups = [[NEAR * k + j for k in range(FAR)] for j in range(NEAR)]
other_chip = [(0, 2), (1, 3), (2, 0), (3, 1)]
other_core = [(0, 1), (1, 0), (2, 3), (3, 2)]

f32, bf16 = jnp.float32, jnp.bfloat16
vmem = pl.BlockSpec(memory_space=pltpu.VMEM)
hbm = pl.BlockSpec(memory_space=pltpu.HBM)
CHUNK = 32
TILE = 256


def to_chip(x):
    return lax.ppermute(x, "mp", other_chip)


def to_core(x):
    return lax.ppermute(x, "mp", other_core)


def shifted(x, axis, by):
    length = lax.axis_size(axis)
    return lax.ppermute(x, axis, [(i, (i + by) % length) for i in range(length)])


def gathered(x, groups):
    copies = jnp.broadcast_to(x, (len(groups[0]), *x.shape))
    return lax.all_to_all(copies, "dp", 0, 0, tiled=True, axis_index_groups=groups)


def exchanged(x, groups):
    return lax.all_to_all(x, "dp", 0, 0, tiled=True, axis_index_groups=groups)


def gelu_both(v):
    t = jnp.tanh(gelu_coef * (v + 0.044715 * v * v * v))
    value = 0.5 * v * (1.0 + t)
    slope = 0.5 * (1.0 + t) + 0.5 * v * (1.0 - t * t) * gelu_coef * (1.0 + 0.134145 * v * v)
    return value, slope


def scale_of(xf):
    return lax.rsqrt(jnp.mean(xf * xf, axis=-1, keepdims=True) + norm_eps)


def nt(a, b):
    return lax.dot_general(a, b, (((1,), (1,)), ((), ())), preferred_element_type=f32)


def tn(a, b):
    return lax.dot_general(a, b, (((0,), (0,)), ((), ())), preferred_element_type=f32)


def nn(a, b):
    return jnp.dot(a, b, preferred_element_type=f32)


def norm_into(src, at, gain, dst, to, rows):
    for r in range(0, rows, CHUNK):
        x = src[at + r : at + r + CHUNK, :].astype(f32)
        dst[to + r : to + r + CHUNK, :] = (x * scale_of(x) * gain[...]).astype(bf16)


def copies_of(pairs, sems):
    copies = [pltpu.make_async_copy(a, b, sems.at[i]) for i, (a, b) in enumerate(pairs)]
    for copy in copies:
        copy.start()
    return copies


def own_kernel(
    xf, xb, ct, near, wi, wo, gain, nf, nb, c2, br, dn, p,
    vx, vnear, vwi, vwo, vbr, vdn, vp, act_f, act, dp, arrived, sent,
):
    rows = xf.shape[0]
    hid = wi.shape[0]
    loads = copies_of(
        [(near, vnear), (xb, vx.at[0]), (xf, vx.at[1]), (ct, c2.at[:rows]), (wi, vwi), (wo, vwo)],
        arrived,
    )
    loads[0].wait()
    norm_into(vnear, rows, gain, nb, rows, rows)
    norm_into(vnear, 0, gain, nf, rows, rows)
    c2[rows:, :] = vnear[2 * rows :, :]
    for load in loads[1:]:
        load.wait()
    norm_into(vx.at[0], 0, gain, nb, 0, rows)
    norm_into(vx.at[1], 0, gain, nf, 0, rows)

    def hidden(j, _):
        h = pl.ds(pl.multiple_of(j * TILE, TILE), TILE)
        value, _ = gelu_both(nt(nf[...], vwi[h, :]))
        act_f[:, h] = value.astype(bf16)
        value, slope = gelu_both(nt(nb[...], vwi[h, :]))
        act[:, h] = value.astype(bf16)
        dp[:, h] = (nt(c2[...], vwo[h, :]) * slope).astype(bf16)

    lax.fori_loop(0, hid // TILE, hidden, None)
    stores = []
    for k in range(FAR):
        c = slice(k * TILE, (k + 1) * TILE)
        vp[c, :hid] = tn(nb[:, c], dp[...]).astype(bf16)
        vp[c, hid:] = tn(c2[:, c], act[...]).astype(bf16)
        store = pltpu.make_async_copy(vp.at[c], p.at[c], sent.at[k])
        store.start()
        stores.append(store)
    for k, (a, w, v, out) in enumerate(((act_f, vwo, vbr, br), (dp, vwi, vdn, dn))):
        for t in range(0, w.shape[1], 2 * TILE):
            v[:, t : t + 2 * TILE] = nn(a[...], w[:, t : t + 2 * TILE]).astype(bf16)
        store = pltpu.make_async_copy(v, out, sent.at[FAR + k])
        store.start()
        stores.append(store)
    for store in stores:
        store.wait()


def rest_kernel(whole, nf, nb, c2, br, dn, keep, send, act_f, dp, wi, wo):
    rows = keep.shape[1]

    def split(i, _):
        r = pl.ds(pl.multiple_of(i * 16, 16), 16)
        wi[r, :] = whole[i, 0]
        wo[r, :] = whole[i, 1]

    lax.fori_loop(0, whole.shape[0], split, None)

    def hidden(j, _):
        h = pl.ds(pl.multiple_of(j * TILE, TILE), TILE)
        value, _ = gelu_both(nt(nf[...], wi[h, :]))
        act_f[:, h] = value.astype(bf16)
        _, slope = gelu_both(nt(nb[...], wi[h, :]))
        dp[:, h] = (nt(c2[...], wo[h, :]) * slope).astype(bf16)

    lax.fori_loop(0, wi.shape[0] // TILE, hidden, None)

    def back(j, _):
        c = pl.ds(pl.multiple_of(j * TILE, TILE), TILE)
        b = br[:, c].astype(f32) + nn(act_f[...], wo[:, c])
        keep[0, :, c] = b[:rows]
        send[0, :, c] = b[rows:].astype(bf16)
        g = dn[:, c].astype(f32) + nn(dp[...], wi[:, c])
        keep[1, :, c] = g[:rows]
        send[1, :, c] = g[rows:].astype(bf16)

    lax.fori_loop(0, wi.shape[1] // TILE, back, None)


def half_kernel(far, far2, wi, gain, nbt, act, slope, vfar, vwi, nb, arrived):
    rows = far.shape[0]
    loads = copies_of([(far, vfar.at[0]), (far2, vfar.at[1]), (wi, vwi)], arrived)
    for k in range(2):
        loads[k].wait()
        norm_into(vfar.at[k], 0, gain, nb, k * rows, rows)
    loads[2].wait()

    def hidden(j, _):
        h = pl.ds(pl.multiple_of(j * TILE, TILE), TILE)
        value, down = gelu_both(nt(nb[...], vwi[h, :]))
        act[:, h] = value.astype(bf16)
        slope[:, h] = down
        for k in range(2):
            c = pl.ds(pl.multiple_of((2 * j + k) * TILE, TILE), TILE)
            nbt[c, :] = nb[:, c].T

    lax.fori_loop(0, wi.shape[0] // TILE, hidden, None)


def grad_kernel(far, far2, wo, nbt, act, slope, p, g, c3, vwo, vnbt, vact, vslope, vp, vg, dp3, arrived, sent):
    rows = far.shape[0]
    hid = wo.shape[0]
    loads = copies_of(
        [
            (far, c3.at[:rows]),
            (far2, c3.at[rows:]),
            (wo, vwo),
            (slope, vslope),
            (act, vact),
            (nbt, vnbt),
            (p, vp),
        ],
        arrived,
    )
    for load in loads[:4]:
        load.wait()

    def hidden(j, _):
        h = pl.ds(pl.multiple_of(j * TILE, TILE), TILE)
        dp3[:, h] = (nt(c3[...], vwo[h, :]) * vslope[:, h]).astype(bf16)

    lax.fori_loop(0, hid // TILE, hidden, None)
    for load in loads[4:]:
        load.wait()
    stores = []
    for k in range(FAR):
        c = slice(k * TILE, (k + 1) * TILE)
        gi = vp[c, :hid].astype(f32) + nn(vnbt[c, :], dp3[...])
        vg[:, k, :, :hid] = gi.astype(bf16).reshape(NEAR, -1, hid)
        go = vp[c, hid:].astype(f32) + tn(c3[:, c], vact[...])
        vg[:, k, :, hid:] = go.astype(bf16).reshape(NEAR, -1, hid)
        store = pltpu.make_async_copy(vg.at[:, k], g.at[:, k], sent.at[k])
        store.start()
        stores.append(store)
    for store in stores:
        store.wait()


def sum_kernel(pieces, total):
    def step(k, _):
        total[k] = jnp.sum(pieces[:, k].astype(f32), axis=0).astype(bf16)

    lax.fori_loop(0, pieces.shape[1], step, None)


def last_kernel(pieces, g_in, g_out):
    hid = g_in.shape[1]
    total = jnp.sum(pieces[...].astype(f32), axis=0).astype(bf16)
    g_in[...] = total[:, :hid]
    g_out[...] = total[:, hid:]


def landed_kernel(a, b, c, d):
    c[0] = a[...]
    d[0] = b[...]


def local(kernel, outs, scratch, flops, moved, mib=62, **specs):
    return pl.pallas_call(
        kernel,
        out_shape=[jax.ShapeDtypeStruct(s, t) for s, t in outs],
        scratch_shapes=[pltpu.VMEM(*a) if isinstance(a, tuple) else a for a in scratch],
        compiler_params=pltpu.CompilerParams(vmem_limit_bytes=mib * 2**20),
        cost_estimate=pl.CostEstimate(flops=flops, bytes_accessed=moved, transcendentals=0),
        **specs,
    )


def layer(fwd_in, stash, cot, w_in, w_out, gain):
    xf, xb, ct = fwd_in[0], stash[0], cot[0]
    wi, wo = w_in[0], w_out[0]
    rows, dim = xf.shape
    hid = wi.shape[0]
    both = 2 * rows
    n_dp = lax.axis_size("dp")
    d = lax.axis_index("dp")
    part = hid // n_dp
    at = (d % NEAR * FAR + d // NEAR) * part
    mine = jnp.stack(
        [lax.dynamic_slice_in_dim(wi, at, part, 0), lax.dynamic_slice_in_dim(wo, at, part, 0)]
    )
    piece = to_chip(mine)
    far_s = to_chip(xb)
    far_c = to_chip(ct)
    near = to_core(jnp.concatenate([xf, xb, ct]))
    dma = pltpu.SemaphoreType.DMA
    nf, nb, c2, br, dn, p = local(
        own_kernel,
        [((both, dim), bf16)] * 5 + [((dim, 2 * hid), bf16)],
        [
            ((2, rows, dim), bf16),
            ((3 * rows, dim), bf16),
            ((hid, dim), bf16),
            ((hid, dim), bf16),
            ((both, dim), bf16),
            ((both, dim), bf16),
            ((dim, 2 * hid), bf16),
            ((both, hid), bf16),
            ((both, hid), bf16),
            ((both, hid), bf16),
            dma((6,)),
            dma((FAR + 2,)),
        ],
        14 * both * hid * dim,
        8 * 2**20,
        in_specs=[hbm] * 6 + [vmem],
        out_specs=[vmem] * 3 + [hbm] * 3,
    )(xf, xb, ct, near, wi, wo, gain)
    col = gathered(piece, far_groups)
    whole = gathered(col, near_groups).reshape(n_dp, 2, part, dim)
    keep, send = local(
        rest_kernel,
        [((2, rows, dim), f32), ((2, rows, dim), bf16)],
        [((both, hid), bf16)] * 2 + [((hid, dim), bf16)] * 2,
        10 * both * hid * dim,
        8 * 2**20,
        mib=56,
    )(whole, nf, nb, c2, br, dn)
    sums = keep + to_core(send).astype(f32)
    out = (xf.astype(f32) + sums[0]).astype(bf16)
    passed_fwd = shifted(out, "section", 1)
    shard_x = xb.astype(f32)
    scale = scale_of(shard_x)
    push = sums[1] * gain
    mixed = jnp.mean(shard_x * push, axis=-1, keepdims=True)
    dx = ct.astype(f32) + scale * push - shard_x * scale * scale * scale * mixed
    passed_grad = shifted(dx.astype(bf16), "section", -1)
    far_s2 = to_core(far_s)
    nbt3, act3, slope3 = local(
        half_kernel,
        [((dim, both), bf16), ((both, hid), bf16), ((both, hid), f32)],
        [((2, rows, dim), bf16), ((hid, dim), bf16), ((both, dim), bf16), dma((3,))],
        2 * both * hid * dim,
        4 * 2**20,
        in_specs=[hbm] * 3 + [vmem],
        out_specs=[vmem] * 3,
    )(far_s, far_s2, wi, gain)
    far_c2 = to_core(far_c)
    cut = dim // n_dp
    (g,) = local(
        grad_kernel,
        [((NEAR, FAR, cut, 2 * hid), bf16)],
        [
            ((both, dim), bf16),
            ((hid, dim), bf16),
            ((dim, both), bf16),
            ((both, hid), bf16),
            ((both, hid), f32),
            ((dim, 2 * hid), bf16),
            ((NEAR, FAR, cut, 2 * hid), bf16),
            ((both, hid), bf16),
            dma((7,)),
            dma((FAR,)),
        ],
        6 * both * hid * dim,
        7 * 2**20,
        in_specs=[hbm] * 7,
        out_specs=[hbm],
    )(far_c, far_c2, wo, nbt3, act3, slope3, p)
    g = exchanged(g, near_groups)
    (g,) = local(sum_kernel, [(g.shape[1:], bf16)], [], 2**21, 2**21, mib=16)(g)
    g = exchanged(g, far_groups)
    passed_fwd, passed_grad = local(
        landed_kernel, [((1, rows, dim), bf16)] * 2, [], 2**20, 2**20, mib=16
    )(passed_fwd, passed_grad)
    g_in, g_out = local(last_kernel, [((cut, hid), bf16)] * 2, [], 2**18, 2**18, mib=16)(g)
    return passed_fwd, passed_grad, g_in.T[None], g_out.T[None]


def solution(mesh):
    in_specs = (
        P("section", ("dp", "mp"), None),
        P("section", ("dp", "mp"), None),
        P("section", ("dp", "mp"), None),
        P("section", "mp", None),
        P("section", "mp", None),
        P("section", None),
    )
    out_specs = (
        P("section", ("dp", "mp"), None),
        P("section", ("dp", "mp"), None),
        P("section", "mp", "dp"),
        P("section", "mp", "dp"),
    )
    return jax.shard_map(
        layer, mesh=mesh, in_specs=in_specs, out_specs=out_specs, check_vma=False
    )
```

```python
import jax
import jax.numpy as jnp
from jax import lax
from jax.experimental import pallas as pl
from jax.experimental.pallas import tpu as pltpu
from jax.sharding import PartitionSpec as P


norm_eps = 1e-05
gelu_coef = 0.7978845608


NEAR, FAR = 8, 4
near_groups = [[NEAR * k + j for j in range(NEAR)] for k in range(FAR)]
far_groups = [[NEAR * k + j for k in range(FAR)] for j in range(NEAR)]
other_chip = [(0, 2), (1, 3), (2, 0), (3, 1)]
other_core = [(0, 1), (1, 0), (2, 3), (3, 2)]

f32, bf16 = jnp.float32, jnp.bfloat16
vmem = pl.BlockSpec(memory_space=pltpu.VMEM)
hbm = pl.BlockSpec(memory_space=pltpu.HBM)
CHUNK = 32
TILE = 256


def to_chip(x):
    return lax.ppermute(x, "mp", other_chip)


def to_core(x):
    return lax.ppermute(x, "mp", other_core)


def shifted(x, axis, by):
    length = lax.axis_size(axis)
    return lax.ppermute(x, axis, [(i, (i + by) % length) for i in range(length)])


def gathered(x, groups):
    copies = jnp.broadcast_to(x, (len(groups[0]), *x.shape))
    return lax.all_to_all(copies, "dp", 0, 0, tiled=True, axis_index_groups=groups)


def exchanged(x, groups):
    return lax.all_to_all(x, "dp", 0, 0, tiled=True, axis_index_groups=groups)


def gelu_both(v):
    t = jnp.tanh(gelu_coef * (v + 0.044715 * v * v * v))
    value = 0.5 * v * (1.0 + t)
    slope = 0.5 * (1.0 + t) + 0.5 * v * (1.0 - t * t) * gelu_coef * (1.0 + 0.134145 * v * v)
    return value, slope


def scale_of(xf):
    return lax.rsqrt(jnp.mean(xf * xf, axis=-1, keepdims=True) + norm_eps)


def nt(a, b):
    return lax.dot_general(a, b, (((1,), (1,)), ((), ())), preferred_element_type=f32)


def tn(a, b):
    return lax.dot_general(a, b, (((0,), (0,)), ((), ())), preferred_element_type=f32)


def nn(a, b):
    return jnp.dot(a, b, preferred_element_type=f32)


def norm_into(src, at, gain, dst, to, rows):
    for r in range(0, rows, CHUNK):
        x = src[at + r : at + r + CHUNK, :].astype(f32)
        dst[to + r : to + r + CHUNK, :] = (x * scale_of(x) * gain[...]).astype(bf16)


def copies_of(pairs, sems):
    copies = [pltpu.make_async_copy(a, b, sems.at[i]) for i, (a, b) in enumerate(pairs)]
    for copy in copies:
        copy.start()
    return copies


def own_kernel(
    xf, xb, ct, near, wi, wo, gain, nf, nb, c2, br, dn, p,
    vx, vnear, vwi, vwo, vbr, vdn, vp, act_f, act, dp, arrived, sent,
):
    rows = xf.shape[0]
    hid = wi.shape[0]
    loads = copies_of(
        [(near, vnear), (xb, vx.at[0]), (xf, vx.at[1]), (ct, c2.at[:rows]), (wi, vwi), (wo, vwo)],
        arrived,
    )
    loads[0].wait()
    norm_into(vnear, rows, gain, nb, rows, rows)
    norm_into(vnear, 0, gain, nf, rows, rows)
    c2[rows:, :] = vnear[2 * rows :, :]
    for load in loads[1:]:
        load.wait()
    norm_into(vx.at[0], 0, gain, nb, 0, rows)
    norm_into(vx.at[1], 0, gain, nf, 0, rows)

    def hidden(j, _):
        h = pl.ds(pl.multiple_of(j * TILE, TILE), TILE)
        value, _ = gelu_both(nt(nf[...], vwi[h, :]))
        act_f[:, h] = value.astype(bf16)
        value, slope = gelu_both(nt(nb[...], vwi[h, :]))
        act[:, h] = value.astype(bf16)
        dp[:, h] = (nt(c2[...], vwo[h, :]) * slope).astype(bf16)

    lax.fori_loop(0, hid // TILE, hidden, None)
    stores = []
    for k in range(FAR):
        c = slice(k * TILE, (k + 1) * TILE)
        vp[c, :hid] = tn(nb[:, c], dp[...]).astype(bf16)
        vp[c, hid:] = tn(c2[:, c], act[...]).astype(bf16)
        store = pltpu.make_async_copy(vp.at[c], p.at[c], sent.at[k])
        store.start()
        stores.append(store)
    for k, (a, w, v, out) in enumerate(((act_f, vwo, vbr, br), (dp, vwi, vdn, dn))):
        for t in range(0, w.shape[1], 2 * TILE):
            v[:, t : t + 2 * TILE] = nn(a[...], w[:, t : t + 2 * TILE]).astype(bf16)
        store = pltpu.make_async_copy(v, out, sent.at[FAR + k])
        store.start()
        stores.append(store)
    for store in stores:
        store.wait()


def rest_kernel(
    whole, nf, nb, c2, br, dn, keep, send, vwi, vwo, vnf, vnb, vc2, vbr, vdn, act_f, dp, arrived
):
    rows = keep.shape[1]
    blocks, part, dim = vwi.shape
    hid = blocks * part
    loads = copies_of(
        [
            (whole.at[:, 0], vwi),
            (nf, vnf),
            (nb, vnb),
            (whole.at[:, 1], vwo),
            (c2, vc2),
            (br, vbr),
            (dn, vdn),
        ],
        arrived,
    )
    for load in loads[:5]:
        load.wait()

    def hidden(j, _):
        h = pl.ds(pl.multiple_of(j * TILE, TILE), TILE)
        of = pl.ds(pl.multiple_of(j * (TILE // part), TILE // part), TILE // part)
        wi = vwi[of].reshape(TILE, dim)
        value, _ = gelu_both(nt(vnf[...], wi))
        act_f[:, h] = value.astype(bf16)
        _, slope = gelu_both(nt(vnb[...], wi))
        dp[:, h] = (nt(vc2[...], vwo[of].reshape(TILE, dim)) * slope).astype(bf16)

    lax.fori_loop(0, hid // TILE, hidden, None)
    for load in loads[5:]:
        load.wait()
    for t in range(0, dim, 2 * TILE):
        c = slice(t, t + 2 * TILE)
        b = vbr[:, c].astype(f32) + nn(act_f[...], vwo[:, :, c].reshape(hid, 2 * TILE))
        keep[0, :, c] = b[:rows]
        send[0, :, c] = b[rows:].astype(bf16)
        g = vdn[:, c].astype(f32) + nn(dp[...], vwi[:, :, c].reshape(hid, 2 * TILE))
        keep[1, :, c] = g[:rows]
        send[1, :, c] = g[rows:].astype(bf16)


def half_kernel(far, far2, wi, gain, nbt, act, slope, vfar, vwi, nb, arrived):
    rows = far.shape[0]
    loads = copies_of([(far, vfar.at[0]), (far2, vfar.at[1]), (wi, vwi)], arrived)
    for k in range(2):
        loads[k].wait()
        norm_into(vfar.at[k], 0, gain, nb, k * rows, rows)
    loads[2].wait()

    def hidden(j, _):
        h = pl.ds(pl.multiple_of(j * TILE, TILE), TILE)
        value, down = gelu_both(nt(nb[...], vwi[h, :]))
        act[:, h] = value.astype(bf16)
        slope[:, h] = down
        for k in range(2):
            c = pl.ds(pl.multiple_of((2 * j + k) * TILE, TILE), TILE)
            nbt[c, :] = nb[:, c].T

    lax.fori_loop(0, wi.shape[0] // TILE, hidden, None)


def grad_kernel(far, far2, wo, nbt, act, slope, p, g, c3, vwo, vnbt, vact, vslope, vp, vg, dp3, arrived, sent):
    rows = far.shape[0]
    hid = wo.shape[0]
    loads = copies_of(
        [
            (far, c3.at[:rows]),
            (far2, c3.at[rows:]),
            (wo, vwo),
            (slope, vslope),
            (act, vact),
            (nbt, vnbt),
            (p, vp),
        ],
        arrived,
    )
    for load in loads[:4]:
        load.wait()

    def hidden(j, _):
        h = pl.ds(pl.multiple_of(j * TILE, TILE), TILE)
        dp3[:, h] = (nt(c3[...], vwo[h, :]) * vslope[:, h]).astype(bf16)

    lax.fori_loop(0, hid // TILE, hidden, None)
    for load in loads[4:]:
        load.wait()
    stores = []
    for k in range(FAR):
        c = slice(k * TILE, (k + 1) * TILE)
        gi = vp[c, :hid].astype(f32) + nn(vnbt[c, :], dp3[...])
        vg[:, k, :, :hid] = gi.astype(bf16).reshape(NEAR, -1, hid)
        go = vp[c, hid:].astype(f32) + tn(c3[:, c], vact[...])
        vg[:, k, :, hid:] = go.astype(bf16).reshape(NEAR, -1, hid)
        store = pltpu.make_async_copy(vg.at[:, k], g.at[:, k], sent.at[k])
        store.start()
        stores.append(store)
    for store in stores:
        store.wait()


def sum_kernel(pieces, total):
    def step(k, _):
        total[k] = jnp.sum(pieces[:, k].astype(f32), axis=0).astype(bf16)

    lax.fori_loop(0, pieces.shape[1], step, None)


def last_kernel(pieces, g_in, g_out):
    hid = g_in.shape[1]
    total = jnp.sum(pieces[...].astype(f32), axis=0).astype(bf16)
    g_in[...] = total[:, :hid]
    g_out[...] = total[:, hid:]


def landed_kernel(a, b, c, d):
    c[0] = a[...]
    d[0] = b[...]


def local(kernel, outs, scratch, flops, moved, mib=62, **specs):
    return pl.pallas_call(
        kernel,
        out_shape=[jax.ShapeDtypeStruct(s, t) for s, t in outs],
        scratch_shapes=[pltpu.VMEM(*a) if isinstance(a, tuple) else a for a in scratch],
        compiler_params=pltpu.CompilerParams(vmem_limit_bytes=mib * 2**20),
        cost_estimate=pl.CostEstimate(flops=flops, bytes_accessed=moved, transcendentals=0),
        **specs,
    )


def layer(fwd_in, stash, cot, w_in, w_out, gain):
    xf, xb, ct = fwd_in[0], stash[0], cot[0]
    wi, wo = w_in[0], w_out[0]
    rows, dim = xf.shape
    hid = wi.shape[0]
    both = 2 * rows
    n_dp = lax.axis_size("dp")
    d = lax.axis_index("dp")
    part = hid // n_dp
    at = (d % NEAR * FAR + d // NEAR) * part
    mine = jnp.stack(
        [lax.dynamic_slice_in_dim(wi, at, part, 0), lax.dynamic_slice_in_dim(wo, at, part, 0)]
    )
    piece = to_chip(mine)
    far_s = to_chip(xb)
    far_c = to_chip(ct)
    near = to_core(jnp.concatenate([xf, xb, ct]))
    dma = pltpu.SemaphoreType.DMA
    nf, nb, c2, br, dn, p = local(
        own_kernel,
        [((both, dim), bf16)] * 5 + [((dim, 2 * hid), bf16)],
        [
            ((2, rows, dim), bf16),
            ((3 * rows, dim), bf16),
            ((hid, dim), bf16),
            ((hid, dim), bf16),
            ((both, dim), bf16),
            ((both, dim), bf16),
            ((dim, 2 * hid), bf16),
            ((both, hid), bf16),
            ((both, hid), bf16),
            ((both, hid), bf16),
            dma((6,)),
            dma((FAR + 2,)),
        ],
        14 * both * hid * dim,
        8 * 2**20,
        in_specs=[hbm] * 6 + [vmem],
        out_specs=[vmem] * 3 + [hbm] * 3,
    )(xf, xb, ct, near, wi, wo, gain)
    col = gathered(piece, far_groups)
    whole = gathered(col, near_groups).reshape(n_dp, 2, part, dim)
    keep, send = local(
        rest_kernel,
        [((2, rows, dim), f32), ((2, rows, dim), bf16)],
        [((n_dp, part, dim), bf16)] * 2
        + [((both, dim), bf16)] * 5
        + [((both, hid), bf16)] * 2
        + [dma((7,))],
        10 * both * hid * dim,
        8 * 2**20,
        mib=56,
        in_specs=[hbm] * 6,
        out_specs=[vmem] * 2,
    )(whole, nf, nb, c2, br, dn)
    sums = keep + to_core(send).astype(f32)
    out = (xf.astype(f32) + sums[0]).astype(bf16)
    passed_fwd = shifted(out, "section", 1)
    shard_x = xb.astype(f32)
    scale = scale_of(shard_x)
    push = sums[1] * gain
    mixed = jnp.mean(shard_x * push, axis=-1, keepdims=True)
    dx = ct.astype(f32) + scale * push - shard_x * scale * scale * scale * mixed
    passed_grad = shifted(dx.astype(bf16), "section", -1)
    far_s2 = to_core(far_s)
    nbt3, act3, slope3 = local(
        half_kernel,
        [((dim, both), bf16), ((both, hid), bf16), ((both, hid), f32)],
        [((2, rows, dim), bf16), ((hid, dim), bf16), ((both, dim), bf16), dma((3,))],
        2 * both * hid * dim,
        4 * 2**20,
        in_specs=[hbm] * 3 + [vmem],
        out_specs=[vmem] * 3,
    )(far_s, far_s2, wi, gain)
    far_c2 = to_core(far_c)
    cut = dim // n_dp
    (g,) = local(
        grad_kernel,
        [((NEAR, FAR, cut, 2 * hid), bf16)],
        [
            ((both, dim), bf16),
            ((hid, dim), bf16),
            ((dim, both), bf16),
            ((both, hid), bf16),
            ((both, hid), f32),
            ((dim, 2 * hid), bf16),
            ((NEAR, FAR, cut, 2 * hid), bf16),
            ((both, hid), bf16),
            dma((7,)),
            dma((FAR,)),
        ],
        6 * both * hid * dim,
        7 * 2**20,
        in_specs=[hbm] * 7,
        out_specs=[hbm],
    )(far_c, far_c2, wo, nbt3, act3, slope3, p)
    g = exchanged(g, near_groups)
    (g,) = local(sum_kernel, [(g.shape[1:], bf16)], [], 2**21, 2**21, mib=16)(g)
    g = exchanged(g, far_groups)
    passed_fwd, passed_grad = local(
        landed_kernel, [((1, rows, dim), bf16)] * 2, [], 2**20, 2**20, mib=16
    )(passed_fwd, passed_grad)
    g_in, g_out = local(last_kernel, [((cut, hid), bf16)] * 2, [], 2**18, 2**18, mib=16)(g)
    return passed_fwd, passed_grad, g_in.T[None], g_out.T[None]


def solution(mesh):
    in_specs = (
        P("section", ("dp", "mp"), None),
        P("section", ("dp", "mp"), None),
        P("section", ("dp", "mp"), None),
        P("section", "mp", None),
        P("section", "mp", None),
        P("section", None),
    )
    out_specs = (
        P("section", ("dp", "mp"), None),
        P("section", ("dp", "mp"), None),
        P("section", "mp", "dp"),
        P("section", "mp", "dp"),
    )
    return jax.shard_map(layer, mesh=mesh, in_specs=in_specs, out_specs=out_specs, check_vma=False)
```
